32 devices in a mesh: band: 8 (over z, y), dir: 4 (over x, core).
Axes of the slice: x: 2, y: 2, z: 4, core: 2. Of those that a mesh axis runs over, the one named last changes fastest.
Arguments:
- visibilities: float32 [8, 2, 2, 2, 16, 512], P('band'), may hold values from -6 to 6
- coherencies: float32 [8, 16, 2, 2, 2, 16, 512], P('band', 'dir'), may hold values from -1.2 to 1.2
- jones_start: float32 [8, 16, 2, 2, 2, 1024], P('band', 'dir'), may hold values from -3.6 to 3.6
- dual_start: float32 [8, 16, 2, 2, 2, 1024], P('band', 'dir'), may hold values from -6 to 6
- consensus_start: float32 [8, 16, 2, 2, 2, 1024], P(None, 'dir'), may hold values from -1.8 to 1.8
- freq_basis: float32 [8, 8], P('band'), may hold values from -1 to 1
- baseline_station_pairs: int32 [2, 512], replicated, may hold values from 0 to 1023
Outputs:
- jones_final: float32 [8, 16, 2, 2, 2, 1024], P('band', 'dir')
- dual_final: float32 [8, 16, 2, 2, 2, 1024], P('band', 'dir')
- consensus_coeffs: float32 [8, 16, 2, 2, 2, 1024], P(None, 'dir')
The draws below stay inside these ranges and needn't reach their ends.
All inputs are finite; a program needn't handle non-finite values.
Results may differ from the reference program's by a relative error of at most 0.0003.
Values sent between devices are 32-bit elements; how exact they have to be, the bound alone decides.
A program may use at most 128 MiB of HBM per device.

```python
import jax
import jax.numpy as jnp
from jax import lax

STATION_COUNT = 1024
TERMS = 8
TIMESLOT_COUNT = 16
BASELINE_COUNT = 512
ITERS = 3
DIRECTION_COUNT = 16
SUBBAND_COUNT = 8


def place_ends(drawn, own_key, least, top_value):
    spot = [jax.random.randint(jax.random.fold_in(own_key, axis), (), 0, length) for axis, length in enumerate(drawn.shape)]
    widest = drawn.shape.index(max(drawn.shape))
    neighbour = spot[:widest] + [(spot[widest] + 1) % drawn.shape[widest]] + spot[widest + 1:]
    return drawn.at[tuple(spot)].set(least).at[tuple(neighbour)].set(top_value)


def block_levels(key, shape, cuts, low, high):
    loudness = 1.0
    for position, shards_of in cuts:
        draws = jax.random.uniform(jax.random.fold_in(jax.random.fold_in(key, 6), position), (shards_of,), jnp.float32, low / len(cuts), high / len(cuts))
        loudness = loudness * jnp.repeat(jnp.exp(draws), shape[position] // shards_of).reshape((-1,) + (1,) * (len(shape) - 1 - position))
    return loudness


def normal_values(own_key, shape, scale, bound, pieces=(), held_as=jnp.bfloat16):
    loudness = block_levels(own_key, shape, pieces, -0.22, 0.18) if pieces else 1.0
    array = jax.random.normal(own_key, shape, jnp.float32) * scale * loudness
    return jnp.minimum(jnp.maximum(array, -bound), bound).astype(held_as)


def setup_inputs(seed: int = 0) -> dict:
    key_of = jax.random.split(jax.random.key(seed), 8)
    visibilities = normal_values(key_of[0], (SUBBAND_COUNT, 2, 2, 2, TIMESLOT_COUNT, BASELINE_COUNT), 1.0, 6.0, ((0, 8),), jnp.float32)
    coherencies = normal_values(key_of[1], (SUBBAND_COUNT, DIRECTION_COUNT, 2, 2, 2, TIMESLOT_COUNT, BASELINE_COUNT), 0.2, 1.2, ((0, 8), (1, 4)), jnp.float32)
    jones_start = normal_values(key_of[2], (SUBBAND_COUNT, DIRECTION_COUNT, 2, 2, 2, STATION_COUNT), 0.6, 3.6, ((0, 8), (1, 4)), jnp.float32)
    dual_start = normal_values(key_of[3], (SUBBAND_COUNT, DIRECTION_COUNT, 2, 2, 2, STATION_COUNT), 1.0, 6.0, ((0, 8), (1, 4)), jnp.float32)
    consensus_start = normal_values(key_of[4], (TERMS, DIRECTION_COUNT, 2, 2, 2, STATION_COUNT), 0.3, 1.8, ((1, 4),), jnp.float32)
    freq_basis = jnp.clip(jax.random.uniform(key_of[5], (SUBBAND_COUNT, TERMS), jnp.float32, -1.0, 1.0) * block_levels(key_of[5], (SUBBAND_COUNT, TERMS), ((0, 8),), -0.4, 0.0), -1.0, 1.0)
    baseline_station_pairs = place_ends(jax.random.randint(key_of[6], (2, BASELINE_COUNT), 0, STATION_COUNT), jax.random.fold_in(key_of[6], 1), 0, STATION_COUNT - 1).astype(jnp.int32)
    return dict(visibilities=visibilities, coherencies=coherencies, jones_start=jones_start, dual_start=dual_start, consensus_start=consensus_start, freq_basis=freq_basis, baseline_station_pairs=baseline_station_pairs)


RHO = 5.0
RIDGE = 0.25

def small_mul(left, right):
    return left[:, 0:1] * right[0:1] + left[:, 1:2] * right[1:2]

def complex_mul(left, right):
    real_part = small_mul(left[0], right[0]) - small_mul(left[1], right[1])
    imag_part = small_mul(left[0], right[1]) + small_mul(left[1], right[0])
    return jnp.stack([real_part, imag_part])

def hermitian(value):
    return jnp.stack([jnp.swapaxes(value[0], 0, 1), -jnp.swapaxes(value[1], 0, 1)])

def solve_right(numer, matrix):
    adjugate = jnp.stack([jnp.stack([matrix[:, 1, 1], -matrix[:, 0, 1]], axis=1), jnp.stack([-matrix[:, 1, 0], matrix[:, 0, 0]], axis=1)], axis=1)
    det_real = matrix[0, 0, 0] * matrix[0, 1, 1] - matrix[1, 0, 0] * matrix[1, 1, 1] - (matrix[0, 0, 1] * matrix[0, 1, 0] - matrix[1, 0, 1] * matrix[1, 1, 0])
    det_imag = matrix[0, 0, 0] * matrix[1, 1, 1] + matrix[1, 0, 0] * matrix[0, 1, 1] - (matrix[0, 0, 1] * matrix[1, 1, 0] + matrix[1, 0, 1] * matrix[0, 1, 0])
    product = complex_mul(numer, adjugate)
    divisor = det_real * det_real + det_imag * det_imag
    real_part = (product[0] * det_real + product[1] * det_imag) / divisor
    imag_part = (product[1] * det_real - product[0] * det_imag) / divisor
    return jnp.stack([real_part, imag_part])

def predict(jones_k, coher_k, first, second):
    jones_first = jnp.take(jones_k, first, axis=-1)[..., None, :]
    jones_second = jnp.take(jones_k, second, axis=-1)[..., None, :]
    return complex_mul(complex_mul(jones_first, coher_k), hermitian(jones_second))

def baseline_terms(target, jones_k, coher_k, first, second):
    jones_first = jnp.take(jones_k, first, axis=-1)[..., None, :]
    jones_second = jnp.take(jones_k, second, axis=-1)[..., None, :]
    along_term = complex_mul(coher_k, hermitian(jones_second))
    back_term = hermitian(complex_mul(jones_first, coher_k))
    flipped = hermitian(target)
    right_first = jnp.sum(complex_mul(target, hermitian(along_term)), axis=-2)
    normal_first = jnp.sum(complex_mul(along_term, hermitian(along_term)), axis=-2)
    right_second = jnp.sum(complex_mul(flipped, hermitian(back_term)), axis=-2)
    normal_second = jnp.sum(complex_mul(back_term, hermitian(back_term)), axis=-2)
    first_part = jnp.concatenate([right_first.reshape(8, -1), normal_first.reshape(8, -1)], axis=0)
    second_part = jnp.concatenate([right_second.reshape(8, -1), normal_second.reshape(8, -1)], axis=0)
    return jnp.concatenate([first_part, second_part], axis=1)

def update_one(right_sum, normal_sum, consensus, dual):
    identity = jnp.stack([jnp.eye(2, dtype=jnp.float32), jnp.zeros((2, 2), jnp.float32)])[..., None]
    matrix = normal_sum + RHO * identity
    return solve_right(right_sum + RHO * consensus - dual, matrix)

def update_band(band_items, first, second):
    vis, coher, jones, dual, consensus = band_items
    stations = jones.shape[-1]
    dirs = jones.shape[0]
    model_terms = jax.vmap(predict, (0, 0, None, None))(jones, coher, first, second)
    residual = vis - jnp.sum(model_terms, axis=0)
    normal_terms = jax.vmap(baseline_terms, (0, 0, 0, None, None))(residual[None] + model_terms, jones, coher, first, second)
    stacked = normal_terms.reshape(dirs * 16, -1)
    segment_ids = jnp.concatenate([first, second]).astype(jnp.int32)
    segment = jax.ops.segment_sum(stacked.T, segment_ids, num_segments=stations).T
    segment = segment.reshape((dirs, 2, 2, 2, 2, stations))
    return jax.vmap(update_one)(segment[:, 0], segment[:, 1], consensus, dual)

def reference(visibilities, coherencies, jones_start, dual_start, consensus_start, freq_basis, baseline_station_pairs):
    first = baseline_station_pairs[0]
    second = baseline_station_pairs[1]
    terms = freq_basis.shape[1]
    gram = jnp.dot(freq_basis.T, freq_basis, precision=lax.Precision.HIGHEST) + RIDGE * freq_basis.shape[0] * jnp.eye(terms, dtype=jnp.float32)
    scale_factor = jnp.linalg.cholesky(gram)
    jones = jones_start
    dual = dual_start
    coeffs = consensus_start
    consensus = jnp.einsum('fm,mkabcs->fkabcs', freq_basis, coeffs, precision=lax.Precision.HIGHEST)
    for turn_index in range(ITERS):
        jones = lax.map(lambda band_items: update_band(band_items, first, second), (visibilities, coherencies, jones, dual, consensus))
        coeff_sums = jnp.einsum('fm,fkabcs->mkabcs', freq_basis, jones + dual / RHO, precision=lax.Precision.HIGHEST)
        flat = coeff_sums.reshape(terms, -1)
        coeffs = jax.scipy.linalg.cho_solve((scale_factor, True), flat).reshape(coeff_sums.shape)
        consensus = jnp.einsum('fm,mkabcs->fkabcs', freq_basis, coeffs, precision=lax.Precision.HIGHEST)
        dual = dual + RHO * (jones - consensus)
    return (jones, dual, coeffs)
```

```python
import functools

import jax
import jax.numpy as jnp
from jax import lax
from jax.experimental import pallas as pl
from jax.experimental.pallas import tpu as pltpu
from jax.sharding import PartitionSpec as P

ITERS = 3
RHO = 5.0
RIDGE = 0.25
LANES = 128
SUB = 8
PIECES = 3
MESH = pl.DeviceIdType.MESH


def cmul(a, b):
    return (a[0] * b[0] - a[1] * b[1], a[0] * b[1] + a[1] * b[0])


def cmul_conj(a, b):
    return (a[0] * b[0] + a[1] * b[1], a[1] * b[0] - a[0] * b[1])


def cadd(a, b):
    return (a[0] + b[0], a[1] + b[1])


def conj(a):
    return (a[0], -a[1])


def re_mul(a, b):
    return a[0] * b[0] - a[1] * b[1]


def scale(r, a):
    return (r * a[0], r * a[1])


def split_store(ref, rows, value):
    left = value
    for piece in range(PIECES):
        part = left.astype(jnp.bfloat16)
        ref[piece * rows : (piece + 1) * rows, :] = part
        if piece + 1 < PIECES:
            left = left - part.astype(jnp.float32)


def join(value, rows):
    total = value[0:rows]
    for piece in range(1, PIECES):
        total = total + value[piece * rows : (piece + 1) * rows]
    return total


def kernel(
    n_band, n_dir, dirs, times, base, stations,
    vis, coh, jones0, dual0, cons0, row, ids_row, ids_col,
    jones, dual, coeffs,
    cons, xall, rows_all, weights, gweights,
    gather_hot, scatter_hot, lhs, lhs_n, ends, grams, cross, vals, vals_n, seg, seg_n,
    model, got_a, sum_a, got_b, sum_b, got_c, res,
    row_send, row_recv, x_send, x_recv, d_send, d_recv,
):
    f32 = jnp.float32
    nrow = 8 * dirs
    per = stations // LANES
    me = lax.axis_index("band")
    mine = lax.axis_index("dir")
    blocks = base // LANES
    halves = times // SUB
    stages = n_dir.bit_length() - 1

    def at(pos):
        half = pos // (n_band // 2)
        return (1 - half) * (2 * pos) + half * (2 * (n_band - 1 - pos) + 1)

    odd = lax.rem(me, 2)
    pos = (1 - odd) * (me // 2) + odd * (n_band - 1 - me // 2)
    nexts = (at(lax.rem(pos + 1, n_band)), at(lax.rem(pos + n_band - 1, n_band)))

    def flip(stage):
        bit = lax.rem(mine // (1 << stage), 2)
        return mine + (1 - 2 * bit) * (1 << stage)

    own = lax.rem(mine, 2)

    barrier = pltpu.get_barrier_semaphore()
    for step in range(1, n_band):
        pl.semaphore_signal(
            barrier, inc=1, device_id={"band": lax.rem(me + step, n_band)}, device_id_type=MESH
        )
    for stage in range(stages):
        pl.semaphore_signal(barrier, inc=1, device_id={"dir": flip(stage)}, device_id_type=MESH)

    step_rows = 32

    def hot_body(i, carry):
        start = pl.multiple_of(i * step_rows, step_rows)
        for j in range(2 * base // LANES):
            lane = slice(j * LANES, (j + 1) * LANES)
            sid = lax.broadcasted_iota(jnp.int32, (step_rows, LANES), 0) + i * step_rows
            same = sid == jnp.broadcast_to(ids_row[0:1, lane], (step_rows, LANES))
            gather_hot[pl.ds(start, step_rows), lane] = jnp.where(same, 1.0, 0.0).astype(jnp.bfloat16)
        return carry

    lax.fori_loop(0, stations // step_rows, hot_body, 0)

    def hot_body2(i, carry):
        start = pl.multiple_of(i * step_rows, step_rows)
        col = ids_col[pl.ds(start, step_rows), :]
        for j in range(stations // LANES):
            lane = slice(j * LANES, (j + 1) * LANES)
            sid = lax.broadcasted_iota(jnp.int32, (step_rows, LANES), 1) + j * LANES
            scatter_hot[pl.ds(start, step_rows), lane] = jnp.where(sid == col, 1.0, 0.0).astype(jnp.bfloat16)
        return carry

    lax.fori_loop(0, 2 * base // step_rows, hot_body2, 0)

    pl.semaphore_wait(barrier, n_band - 1 + stages)

    row_copies = []
    for step in range(1, n_band):
        copy = pltpu.make_async_remote_copy(
            src_ref=row,
            dst_ref=rows_all.at[step],
            send_sem=row_send.at[step],
            recv_sem=row_recv.at[step],
            device_id={"band": lax.rem(me + step, n_band)},
            device_id_type=MESH,
        )
        copy.start()
        row_copies.append(copy)

    cons[...] = cons0[...]
    dual[...] = dual0[...]

    pairs = [(a, b) for a in range(4) for b in range(a, 4)]

    def gram_body(j, carry):
        lane = pl.ds(pl.multiple_of(j * LANES, LANES), LANES)
        for k in range(dirs):
            c = [
                [coh[k, v, h * SUB : (h + 1) * SUB, lane] for h in range(halves)]
                for v in range(8)
            ]
            for n, (a, b) in enumerate(pairs):
                real = sum(c[a][h] * c[b][h] + c[4 + a][h] * c[4 + b][h] for h in range(halves))
                grams[(2 * n) * dirs + k : (2 * n) * dirs + k + 1, lane] = jnp.sum(real, axis=0, keepdims=True)
                if a != b:
                    imag = sum(c[4 + a][h] * c[b][h] - c[a][h] * c[4 + b][h] for h in range(halves))
                    grams[(2 * n + 1) * dirs + k : (2 * n + 1) * dirs + k + 1, lane] = jnp.sum(
                        imag, axis=0, keepdims=True
                    )
        return carry

    lax.fori_loop(0, blocks, gram_body, 0)

    def gram(a, b):
        if a > b:
            return conj(gram(b, a))
        n = pairs.index((a, b))
        real = grams[(2 * n) * dirs : (2 * n + 1) * dirs, :]
        if a == b:
            return real
        return (real, grams[(2 * n + 1) * dirs : (2 * n + 2) * dirs, :])

    def solve_weights():
        for copy in row_copies:
            copy.wait()
        rows_all[0] = row[...]
        held = [rows_all[s] for s in range(n_band)]
        columns = []
        for m in range(SUB):
            total = held[0] * held[0][m : m + 1, :]
            for s in range(1, n_band):
                total = total + held[s] * held[s][m : m + 1, :]
            ident = jnp.where(lax.broadcasted_iota(jnp.int32, (SUB, LANES), 0) == m, RIDGE * n_band, 0.0)
            columns.append(total + ident.astype(f32))
        right = list(held)
        iota = lax.broadcasted_iota(jnp.int32, (SUB, LANES), 0)
        for i in range(SUB):
            inverse = 1.0 / columns[i][i : i + 1, :]
            factor = columns[i]
            for group in (columns, right):
                for c in range(len(group)):
                    lead = jnp.broadcast_to(group[c][i : i + 1, :] * inverse, (SUB, LANES))
                    group[c] = jnp.where(iota == i, lead, group[c] - factor * lead)
        for s in range(n_band):
            band = lax.rem(me + n_band - s, n_band)
            gweights[band] = right[s]
            weights[band] = jnp.broadcast_to(
                jnp.sum(right[s] * held[0], axis=0, keepdims=True), (SUB, LANES)
            )

    x_copies = [{} for _ in range(ITERS)]

    def send_x(turn, k, slot):
        copy = pltpu.make_async_remote_copy(
            src_ref=xall.at[turn, k, slot],
            dst_ref=xall.at[turn, k, slot + 1],
            send_sem=x_send.at[turn, k, slot],
            recv_sem=x_recv.at[turn, k, slot],
            device_id={"band": nexts[k % 2]},
            device_id_type=MESH,
        )
        copy.start()
        x_copies[turn][(k, slot)] = copy

    def pump(turn, slot):
        for k in range(dirs):
            x_copies[turn][(k, slot - 1)].wait_recv()
            if slot < n_band - 1:
                send_x(turn, k, slot)

    def source(k, slot):
        if k % 2 == 0:
            return at(lax.rem(pos + n_band - slot, n_band))
        return at(lax.rem(pos + slot, n_band))

    def end(comp, lane):
        return ends[comp * dirs : (comp + 1) * dirs, lane]

    d_copies = []

    def send_d(turn, n, src, dst, stage):
        copy = pltpu.make_async_remote_copy(
            src_ref=src,
            dst_ref=dst,
            send_sem=d_send.at[turn, n],
            recv_sem=d_recv.at[turn, n],
            device_id={"dir": flip(stage)},
            device_id_type=MESH,
        )
        copy.start()
        d_copies.append(copy)
        return copy

    first = slice(0, base)
    second = slice(base, 2 * base)

    for turn in range(ITERS):
        start_ref = jones0 if turn == 0 else jones
        for g in range(nrow // SUB):
            for j in range(per):
                value = start_ref[pl.ds(g * SUB * per + j, SUB, stride=per), :]
                left = value
                for piece in range(PIECES):
                    part = left.astype(jnp.bfloat16)
                    lhs[
                        piece * nrow + g * SUB : piece * nrow + (g + 1) * SUB,
                        j * LANES : (j + 1) * LANES,
                    ] = part
                    left = left - part.astype(f32)
        ends[...] = join(jnp.dot(lhs[...], gather_hot[...], preferred_element_type=f32), nrow)

        def model_body(i, carry):
            j = i // halves
            h = lax.rem(i, halves)
            lane = pl.ds(pl.multiple_of(j * LANES, LANES), LANES)
            lane_q = pl.ds(pl.multiple_of(base + j * LANES, LANES), LANES)
            time = pl.ds(pl.multiple_of(h * SUB, SUB), SUB)
            total = [None] * 4
            for k in range(dirs):
                c = [(coh[k, v, time, lane], coh[k, 4 + v, time, lane]) for v in range(4)]

                def spread(v, where):
                    return tuple(
                        jnp.broadcast_to(
                            ends[(4 * part + v) * dirs + k : (4 * part + v) * dirs + k + 1, where],
                            (SUB, LANES),
                        )
                        for part in range(2)
                    )

                p = [spread(v, lane) for v in range(4)]
                q = [spread(v, lane_q) for v in range(4)]
                for a in range(2):
                    b = [cadd(cmul(p[2 * a], c[d]), cmul(p[2 * a + 1], c[2 + d])) for d in range(2)]
                    for d in range(2):
                        term = cadd(cmul_conj(b[0], q[2 * d]), cmul_conj(b[1], q[2 * d + 1]))
                        v = 2 * a + d
                        total[v] = term if total[v] is None else cadd(total[v], term)
            for v in range(4):
                model[turn, 0, v, time, lane] = total[v][0]
                model[turn, 1, v, time, lane] = total[v][1]
            return carry

        lax.fori_loop(0, blocks * halves, model_body, 0)

        other = 1 - own
        hop = send_d(turn, 0, model.at[turn, other], got_a.at[turn], 0)
        if turn > 0:
            pump(turn - 1, 1)

        jp = [(end(v, first), end(4 + v, first)) for v in range(4)]
        jq = [(end(v, second), end(4 + v, second)) for v in range(4)]

        def gram_of(j):
            m00 = re_mul(j[0], conj(j[0])) + re_mul(j[2], conj(j[2]))
            m11 = re_mul(j[1], conj(j[1])) + re_mul(j[3], conj(j[3]))
            m01 = cadd(cmul_conj(j[1], j[0]), cmul_conj(j[3], j[2]))
            return m00, m11, m01

        m00, m11, m01 = gram_of(jq)
        p00, p11, p01 = gram_of(jp)
        n1_00 = m00 * gram(0, 0) + m11 * gram(1, 1) + 2.0 * re_mul(m01, gram(0, 1))
        n1_11 = m00 * gram(2, 2) + m11 * gram(3, 3) + 2.0 * re_mul(m01, gram(2, 3))
        n1_01 = cadd(
            cadd(scale(m00, gram(0, 2)), scale(m11, gram(1, 3))),
            cadd(cmul(m01, gram(0, 3)), cmul(conj(m01), gram(1, 2))),
        )
        n2_00 = p00 * gram(0, 0) + p11 * gram(2, 2) + 2.0 * re_mul(p01, gram(2, 0))
        n2_11 = p00 * gram(1, 1) + p11 * gram(3, 3) + 2.0 * re_mul(p01, gram(3, 1))
        n2_01 = cadd(
            cadd(scale(p00, gram(1, 0)), scale(p11, gram(3, 2))),
            cadd(cmul(p01, gram(3, 0)), cmul(conj(p01), gram(1, 2))),
        )
        for n, (left, right) in enumerate(
            ((n1_00, n2_00), (n1_11, n2_11), (n1_01[0], n2_01[0]), (n1_01[1], n2_01[1]))
        ):
            vals_n[n * dirs : (n + 1) * dirs, first] = left
            vals_n[n * dirs : (n + 1) * dirs, second] = right

        hop.wait_recv()
        sum_a[turn, 0] = model[turn, own] + got_a[turn]
        for stage in range(1, stages):
            hop = send_d(turn, stage, sum_a.at[turn, stage - 1], got_b.at[turn, stage - 1], stage)
            if stage == 1:
                split_store(lhs_n, 4 * dirs, vals_n[...])
                found = join(jnp.dot(lhs_n[...], scatter_hot[...], preferred_element_type=f32), 4 * dirs)
                for g in range(4 * dirs // SUB):
                    for j in range(per):
                        seg_n[pl.ds(g * SUB * per + j, SUB, stride=per), :] = found[
                            g * SUB : (g + 1) * SUB, j * LANES : (j + 1) * LANES
                        ]
                if turn == 0:
                    solve_weights()
                else:
                    for s in range(2, n_band // 2):
                        pump(turn - 1, s)
            hop.wait_recv()
            target = sum_a.at[turn, stage] if stage + 1 < stages else sum_b.at[turn]
            target[...] = sum_a[turn, stage - 1] + got_b[turn, stage - 1]
        hop = send_d(turn, stages, sum_b.at[turn], got_c.at[turn], 0)
        if turn > 0:
            pump(turn - 1, n_band // 2)
        res[own] = vis[own] - sum_b[turn]
        hop.wait_recv()
        res[other] = vis[other] - got_c[turn]

        def cross_body(j, carry):
            lane = pl.ds(pl.multiple_of(j * LANES, LANES), LANES)
            r = [[res[v // 4, v % 4, h * SUB : (h + 1) * SUB, lane] for h in range(halves)] for v in range(8)]
            for k in range(dirs):
                c = [[coh[k, v, h * SUB : (h + 1) * SUB, lane] for h in range(halves)] for v in range(8)]
                for a in range(4):
                    for b in range(4):
                        real = sum(r[a][h] * c[b][h] + r[4 + a][h] * c[4 + b][h] for h in range(halves))
                        imag = sum(r[4 + a][h] * c[b][h] - r[a][h] * c[4 + b][h] for h in range(halves))
                        n = 2 * (4 * a + b)
                        cross[n * dirs + k : n * dirs + k + 1, lane] = jnp.sum(real, axis=0, keepdims=True)
                        cross[(n + 1) * dirs + k : (n + 1) * dirs + k + 1, lane] = jnp.sum(
                            imag, axis=0, keepdims=True
                        )
            return carry

        lax.fori_loop(0, blocks, cross_body, 0)

        if turn > 0:
            for s in range(n_band // 2 + 1, n_band - 1):
                pump(turn - 1, s)

        def crossed(a, b):
            n = 2 * (4 * a + b)
            return (
                cross[n * dirs : (n + 1) * dirs, :],
                cross[(n + 1) * dirs : (n + 2) * dirs, :],
            )

        def herm(which):
            zero = [vals_n[n * dirs : (n + 1) * dirs, which] for n in range(4)]
            return zero[0], zero[1], (zero[2], zero[3])

        for which, j, other_end in ((first, jq, jp), (second, jp, jq)):
            h00, h11, h01 = herm(which)
            for a in range(2):
                for c in range(2):
                    total = None
                    for b in range(2):
                        for d in range(2):
                            if which is first:
                                term = cmul(j[2 * b + d], crossed(2 * a + b, 2 * c + d))
                            else:
                                term = cmul_conj(j[2 * b + d], crossed(2 * b + a, 2 * d + c))
                            total = term if total is None else cadd(total, term)
                    if c == 0:
                        extra = cadd(scale(h00, other_end[2 * a]), cmul_conj(other_end[2 * a + 1], h01))
                    else:
                        extra = cadd(cmul(other_end[2 * a], h01), scale(h11, other_end[2 * a + 1]))
                    total = cadd(total, extra)
                    for part in range(2):
                        n = 4 * part + 2 * a + c
                        vals[n * dirs : (n + 1) * dirs, which] = total[part]

        split_store(lhs, nrow, vals[...])
        found = join(jnp.dot(lhs[...], scatter_hot[...], preferred_element_type=f32), nrow)
        for g in range(nrow // SUB):
            for j in range(per):
                seg[pl.ds(g * SUB * per + j, SUB, stride=per), :] = found[
                    g * SUB : (g + 1) * SUB, j * LANES : (j + 1) * LANES
                ]

        def join_bands(previous):
            pump(previous, n_band - 1)
            for k in range(dirs):
                for v in range(8):
                    here = pl.ds((v * dirs + k) * per, per)
                    total = None
                    for s in range(n_band):
                        term = weights[source(k, s)] * xall[previous, k, s, v]
                        total = term if total is None else total + term
                    cons[here, :] = total
                    dual[here, :] = dual[here, :] + RHO * (jones[here, :] - total)

        if turn > 0:
            join_bands(turn - 1)

        for k in range(dirs):
            def rows_of(v):
                return pl.ds((v * dirs + k) * per, per)

            y = []
            for v in range(8):
                here = rows_of(v)
                y.append(seg[here, :] + RHO * cons[here, :] - dual[here, :])
            h00, h11, re01, im01 = [seg_n[rows_of(n), :] for n in range(4)]
            h00 = h00 + RHO
            h11 = h11 + RHO
            inverse = 1.0 / (h00 * h11 - (re01 * re01 + im01 * im01))
            h00, h11, h01 = h00 * inverse, h11 * inverse, (re01 * inverse, im01 * inverse)
            for a in range(2):
                y0, y1 = (y[2 * a], y[4 + 2 * a]), (y[2 * a + 1], y[4 + 2 * a + 1])
                minus0, minus1 = cmul_conj(y1, h01), cmul(y0, h01)
                for part in range(2):
                    for c in range(2):
                        if c == 0:
                            value = h11 * y0[part] - minus0[part]
                        else:
                            value = h00 * y1[part] - minus1[part]
                        v = 4 * part + 2 * a + c
                        here = rows_of(v)
                        jones[here, :] = value
                        xall[turn, k, 0, v] = value + dual[here, :] * (1.0 / RHO)
            send_x(turn, k, 0)

    last = ITERS - 1
    for s in range(1, n_band - 1):
        pump(last, s)
    join_bands(last)

    def coeff_body(m, carry):
        for k in range(dirs):
            total = [None] * 8
            for s in range(n_band):
                factor = jnp.broadcast_to(gweights[source(k, s), pl.ds(m, 1), :], (SUB, LANES))
                for v in range(8):
                    term = factor * xall[last, k, s, v]
                    total[v] = term if total[v] is None else total[v] + term
            for v in range(8):
                coeffs[m, k, v] = total[v]
        return carry

    lax.fori_loop(0, SUB, coeff_body, 0)

    for copies in x_copies:
        for copy in copies.values():
            copy.wait_send()
    for copy in d_copies:
        copy.wait_send()


def local(n_band, n_dir, vis, coh, jones_start, dual_start, consensus_start, freq_basis, pairs):
    f32 = jnp.float32
    dirs, times, base = coh.shape[1], coh.shape[-2], coh.shape[-1]
    stations = jones_start.shape[-1]
    per = stations // LANES
    nrow = 8 * dirs
    terms = freq_basis.shape[1]

    def pack(value):
        value = value.reshape(dirs, 8, per, LANES)
        return jnp.swapaxes(value, 0, 1).reshape(nrow * per, LANES)

    def unpack(value):
        value = value.reshape(8, dirs, per, LANES)
        return jnp.swapaxes(value, 0, 1).reshape(jones_start.shape)

    row = freq_basis[0]
    cons0 = jnp.sum(row.reshape((terms,) + (1,) * 5) * consensus_start, axis=0)
    ids = pairs.reshape(-1)
    stages = n_dir.bit_length() - 1
    half = (4, times, base)
    vmem = pl.BlockSpec(memory_space=pltpu.VMEM)
    packed = jax.ShapeDtypeStruct((nrow * per, LANES), f32)
    bf16 = jnp.bfloat16
    jones, dual, coeffs = pl.pallas_call(
        functools.partial(kernel, n_band, n_dir, dirs, times, base, stations),
        out_shape=(packed, packed, jax.ShapeDtypeStruct((terms, dirs, 8, per, LANES), f32)),
        in_specs=[vmem] * 8,
        out_specs=(vmem,) * 3,
        scratch_shapes=[
            pltpu.VMEM((nrow * per, LANES), f32),
            pltpu.VMEM((ITERS, dirs, n_band, 8, per, LANES), f32),
            pltpu.VMEM((n_band, SUB, LANES), f32),
            pltpu.VMEM((n_band, SUB, LANES), f32),
            pltpu.VMEM((n_band, SUB, LANES), f32),
            pltpu.VMEM((stations, 2 * base), bf16),
            pltpu.VMEM((2 * base, stations), bf16),
            pltpu.VMEM((PIECES * nrow, max(stations, 2 * base)), bf16),
            pltpu.VMEM((PIECES * 4 * dirs, 2 * base), bf16),
            pltpu.VMEM((nrow, 2 * base), f32),
            pltpu.VMEM((20 * dirs, base), f32),
            pltpu.VMEM((32 * dirs, base), f32),
            pltpu.VMEM((nrow, 2 * base), f32),
            pltpu.VMEM((4 * dirs, 2 * base), f32),
            pltpu.VMEM((nrow * per, LANES), f32),
            pltpu.VMEM((4 * dirs * per, LANES), f32),
            pltpu.VMEM((ITERS, 2) + half, f32),
            pltpu.VMEM((ITERS,) + half, f32),
            pltpu.VMEM((ITERS, stages - 1) + half, f32),
            pltpu.VMEM((ITERS, stages - 1) + half, f32),
            pltpu.VMEM((ITERS,) + half, f32),
            pltpu.VMEM((ITERS,) + half, f32),
            pltpu.VMEM((2,) + half, f32),
            pltpu.SemaphoreType.DMA((n_band,)),
            pltpu.SemaphoreType.DMA((n_band,)),
            pltpu.SemaphoreType.DMA((ITERS, dirs, n_band - 1)),
            pltpu.SemaphoreType.DMA((ITERS, dirs, n_band - 1)),
            pltpu.SemaphoreType.DMA((ITERS, stages + 1)),
            pltpu.SemaphoreType.DMA((ITERS, stages + 1)),
        ],
        compiler_params=pltpu.CompilerParams(
            collective_id=0, has_side_effects=True, vmem_limit_bytes=60 * 1024 * 1024
        ),
    )(
        vis.reshape((2,) + half),
        coh.reshape(dirs, 8, times, base),
        pack(jones_start),
        pack(dual_start),
        pack(cons0),
        jnp.broadcast_to(row[:, None], (terms, LANES)),
        ids.reshape(1, -1),
        jnp.broadcast_to(ids[:, None], (2 * base, LANES)),
    )
    coeffs = coeffs.reshape(consensus_start.shape)
    return unpack(jones), unpack(dual), coeffs


def solution(mesh):
    in_specs = (
        P("band", None, None, None, None, None),
        P("band", "dir", None, None, None, None, None),
        P("band", "dir", None, None, None, None),
        P("band", "dir", None, None, None, None),
        P(None, "dir", None, None, None, None),
        P("band", None),
        P(),
    )
    out_specs = (
        P("band", "dir", None, None, None, None),
        P("band", "dir", None, None, None, None),
        P(None, "dir", None, None, None, None),
    )
    body = functools.partial(local, mesh.shape["band"], mesh.shape["dir"])
    return jax.shard_map(body, mesh=mesh, in_specs=in_specs, out_specs=out_specs, check_vma=False)
```

```python
import functools

import jax
import jax.numpy as jnp
from jax import lax
from jax.experimental import pallas as pl
from jax.experimental.pallas import tpu as pltpu
from jax.sharding import PartitionSpec as P

ITERS = 3
RHO = 5.0
RIDGE = 0.25
LANES = 128
SUB = 8
PIECES = 3
MESH = pl.DeviceIdType.MESH


def cmul(a, b):
    return (a[0] * b[0] - a[1] * b[1], a[0] * b[1] + a[1] * b[0])


def cmul_conj(a, b):
    return (a[0] * b[0] + a[1] * b[1], a[1] * b[0] - a[0] * b[1])


def cadd(a, b):
    return (a[0] + b[0], a[1] + b[1])


def conj(a):
    return (a[0], -a[1])


def re_mul(a, b):
    return a[0] * b[0] - a[1] * b[1]


def scale(r, a):
    return (r * a[0], r * a[1])


def split_store(ref, rows, value):
    left = value
    for piece in range(PIECES):
        part = left.astype(jnp.bfloat16)
        ref[piece * rows : (piece + 1) * rows, :] = part
        if piece + 1 < PIECES:
            left = left - part.astype(jnp.float32)


def join(value, rows):
    total = value[0:rows]
    for piece in range(1, PIECES):
        total = total + value[piece * rows : (piece + 1) * rows]
    return total


def kernel(
    n_band, n_dir, dirs, times, base, stations,
    vis_far, coh_far, jones0, dual0, coeffs0_far, basis, pairs_ref,
    jones_out, dual_out, coeffs,
    vis, coh, coeffs0, jones, dual, row, ids_col,
    cons, xall, rows_all, weights, gweights,
    gather_hot, scatter_hot, lhs, lhs_n, ends, grams, cross, vals, vals_n, seg, seg_n,
    model, got_a, sum_a, got_b, sum_b, got_c, res,
    load_sem, row_send, row_recv, x_send, x_recv, d_send, d_recv,
):
    f32 = jnp.float32
    nrow = 8 * dirs
    per = stations // LANES
    me = lax.axis_index("band")
    mine = lax.axis_index("dir")
    blocks = base // LANES
    halves = times // SUB
    stages = n_dir.bit_length() - 1

    def at(pos):
        half = pos // (n_band // 2)
        return (1 - half) * (2 * pos) + half * (2 * (n_band - 1 - pos) + 1)

    odd = lax.rem(me, 2)
    pos = (1 - odd) * (me // 2) + odd * (n_band - 1 - me // 2)
    nexts = (at(lax.rem(pos + 1, n_band)), at(lax.rem(pos + n_band - 1, n_band)))

    def flip(stage):
        bit = lax.rem(mine // (1 << stage), 2)
        return mine + (1 - 2 * bit) * (1 << stage)

    own = lax.rem(mine, 2)

    loads = []
    for n, (far, near) in enumerate(((coh_far, coh), (vis_far, vis), (coeffs0_far, coeffs0))):
        loads.append(pltpu.make_async_copy(far, near, load_sem.at[n]))
        loads[-1].start()

    barrier = pltpu.get_barrier_semaphore()
    for step in range(1, n_band):
        pl.semaphore_signal(
            barrier, inc=1, device_id={"band": lax.rem(me + step, n_band)}, device_id_type=MESH
        )
    for stage in range(stages):
        pl.semaphore_signal(barrier, inc=1, device_id={"dir": flip(stage)}, device_id_type=MESH)

    def halves_of(k, v):
        return (k, v // 2, pl.ds(v % 2, per, stride=2), slice(None))

    def packed(k, v):
        return pl.ds((v * dirs + k) * per, per)

    row[...] = jnp.zeros((SUB, LANES), f32)
    for m in range(SUB):
        row[m : m + 1, :] = jnp.full((1, LANES), basis[0, m], f32)
    for k in range(dirs):
        for v in range(8):
            jones[packed(k, v), :] = jones0[halves_of(k, v)]
            dual[packed(k, v), :] = dual0[halves_of(k, v)]

    for j in range(2 * base // LANES):
        lane = (j * LANES) % base
        which = (j * LANES) // base
        ids = jnp.broadcast_to(pairs_ref[which : which + 1, lane : lane + LANES], (LANES, LANES))
        ids_col[j * LANES : (j + 1) * LANES, :] = jnp.transpose(ids)
    step_rows = 32

    def hot_body(i, carry):
        start = pl.multiple_of(i * step_rows, step_rows)
        for j in range(2 * base // LANES):
            lane = slice(j * LANES, (j + 1) * LANES)
            sid = lax.broadcasted_iota(jnp.int32, (step_rows, LANES), 0) + i * step_rows
            which, low = (j * LANES) // base, (j * LANES) % base
            ids = pairs_ref[which : which + 1, low : low + LANES]
            same = sid == jnp.broadcast_to(ids, (step_rows, LANES))
            gather_hot[pl.ds(start, step_rows), lane] = jnp.where(same, 1.0, 0.0).astype(jnp.bfloat16)
        return carry

    lax.fori_loop(0, stations // step_rows, hot_body, 0)

    def hot_body2(i, carry):
        start = pl.multiple_of(i * step_rows, step_rows)
        col = ids_col[pl.ds(start, step_rows), :]
        for j in range(stations // LANES):
            lane = slice(j * LANES, (j + 1) * LANES)
            sid = lax.broadcasted_iota(jnp.int32, (step_rows, LANES), 1) + j * LANES
            scatter_hot[pl.ds(start, step_rows), lane] = jnp.where(sid == col, 1.0, 0.0).astype(jnp.bfloat16)
        return carry

    lax.fori_loop(0, 2 * base // step_rows, hot_body2, 0)

    pl.semaphore_wait(barrier, n_band - 1 + stages)

    row_copies = []
    for step in range(1, n_band):
        copy = pltpu.make_async_remote_copy(
            src_ref=row,
            dst_ref=rows_all.at[step],
            send_sem=row_send.at[step],
            recv_sem=row_recv.at[step],
            device_id={"band": lax.rem(me + step, n_band)},
            device_id_type=MESH,
        )
        copy.start()
        row_copies.append(copy)

    loads[0].wait()

    pairs = [(a, b) for a in range(4) for b in range(a, 4)]

    def gram_body(j, carry):
        lane = pl.ds(pl.multiple_of(j * LANES, LANES), LANES)
        for k in range(dirs):
            c = [
                [coh[k, v, h * SUB : (h + 1) * SUB, lane] for h in range(halves)]
                for v in range(8)
            ]
            for n, (a, b) in enumerate(pairs):
                real = sum(c[a][h] * c[b][h] + c[4 + a][h] * c[4 + b][h] for h in range(halves))
                grams[(2 * n) * dirs + k : (2 * n) * dirs + k + 1, lane] = jnp.sum(real, axis=0, keepdims=True)
                if a != b:
                    imag = sum(c[4 + a][h] * c[b][h] - c[a][h] * c[4 + b][h] for h in range(halves))
                    grams[(2 * n + 1) * dirs + k : (2 * n + 1) * dirs + k + 1, lane] = jnp.sum(
                        imag, axis=0, keepdims=True
                    )
        return carry

    lax.fori_loop(0, blocks, gram_body, 0)

    def gram(a, b):
        if a > b:
            return conj(gram(b, a))
        n = pairs.index((a, b))
        real = grams[(2 * n) * dirs : (2 * n + 1) * dirs, :]
        if a == b:
            return real
        return (real, grams[(2 * n + 1) * dirs : (2 * n + 2) * dirs, :])

    def start_consensus():
        loads[1].wait()
        loads[2].wait()
        for k in range(dirs):
            for v in range(8):
                total = basis[0, 0] * coeffs0[(0,) + halves_of(k, v)]
                for m in range(1, SUB):
                    total = total + basis[0, m] * coeffs0[(m,) + halves_of(k, v)]
                cons[packed(k, v), :] = total

    def solve_weights():
        for copy in row_copies:
            copy.wait()
        rows_all[0] = row[...]
        held = [rows_all[s] for s in range(n_band)]
        columns = []
        for m in range(SUB):
            total = held[0] * held[0][m : m + 1, :]
            for s in range(1, n_band):
                total = total + held[s] * held[s][m : m + 1, :]
            ident = jnp.where(lax.broadcasted_iota(jnp.int32, (SUB, LANES), 0) == m, RIDGE * n_band, 0.0)
            columns.append(total + ident.astype(f32))
        right = list(held)
        iota = lax.broadcasted_iota(jnp.int32, (SUB, LANES), 0)
        for i in range(SUB):
            inverse = 1.0 / columns[i][i : i + 1, :]
            factor = columns[i]
            for group in (columns, right):
                for c in range(len(group)):
                    lead = jnp.broadcast_to(group[c][i : i + 1, :] * inverse, (SUB, LANES))
                    group[c] = jnp.where(iota == i, lead, group[c] - factor * lead)
        for s in range(n_band):
            band = lax.rem(me + n_band - s, n_band)
            gweights[band] = right[s]
            weights[band] = jnp.broadcast_to(
                jnp.sum(right[s] * held[0], axis=0, keepdims=True), (SUB, LANES)
            )

    x_copies = [{} for _ in range(ITERS)]

    ahead = n_band // 2
    behind = n_band - 1 - ahead

    def slot_of(way, distance):
        return distance if way == 0 or distance == 0 else ahead + distance

    def send_x(turn, k, way, distance):
        to = slot_of(way, distance + 1)
        copy = pltpu.make_async_remote_copy(
            src_ref=xall.at[turn, k, slot_of(way, distance)],
            dst_ref=xall.at[turn, k, to],
            send_sem=x_send.at[turn, k, to - 1],
            recv_sem=x_recv.at[turn, k, to - 1],
            device_id={"band": nexts[way]},
            device_id_type=MESH,
        )
        copy.start()
        x_copies[turn][(k, way, distance + 1)] = copy

    def pump(turn, distance):
        for k in range(dirs):
            for way, reach in enumerate((ahead, behind)):
                if distance <= reach:
                    x_copies[turn][(k, way, distance)].wait_recv()
                    if distance < reach:
                        send_x(turn, k, way, distance)

    def source(slot):
        if slot <= ahead:
            return at(lax.rem(pos + n_band - slot, n_band))
        return at(lax.rem(pos + slot - ahead, n_band))

    def end(comp, lane):
        return ends[comp * dirs : (comp + 1) * dirs, lane]

    d_copies = []

    def send_d(turn, n, src, dst, stage):
        copy = pltpu.make_async_remote_copy(
            src_ref=src,
            dst_ref=dst,
            send_sem=d_send.at[turn, n],
            recv_sem=d_recv.at[turn, n],
            device_id={"dir": flip(stage)},
            device_id_type=MESH,
        )
        copy.start()
        d_copies.append(copy)
        return copy

    first = slice(0, base)
    second = slice(base, 2 * base)

    for turn in range(ITERS):
        for g in range(nrow // SUB):
            for j in range(per):
                value = jones[pl.ds(g * SUB * per + j, SUB, stride=per), :]
                left = value
                for piece in range(PIECES):
                    part = left.astype(jnp.bfloat16)
                    lhs[
                        piece * nrow + g * SUB : piece * nrow + (g + 1) * SUB,
                        j * LANES : (j + 1) * LANES,
                    ] = part
                    left = left - part.astype(f32)
        ends[...] = join(jnp.dot(lhs[...], gather_hot[...], preferred_element_type=f32), nrow)

        def model_body(i, carry):
            j = i // halves
            h = lax.rem(i, halves)
            lane = pl.ds(pl.multiple_of(j * LANES, LANES), LANES)
            lane_q = pl.ds(pl.multiple_of(base + j * LANES, LANES), LANES)
            time = pl.ds(pl.multiple_of(h * SUB, SUB), SUB)
            total = [None] * 4
            for k in range(dirs):
                c = [(coh[k, v, time, lane], coh[k, 4 + v, time, lane]) for v in range(4)]

                def spread(v, where):
                    return tuple(
                        jnp.broadcast_to(
                            ends[(4 * part + v) * dirs + k : (4 * part + v) * dirs + k + 1, where],
                            (SUB, LANES),
                        )
                        for part in range(2)
                    )

                p = [spread(v, lane) for v in range(4)]
                q = [spread(v, lane_q) for v in range(4)]
                for a in range(2):
                    b = [cadd(cmul(p[2 * a], c[d]), cmul(p[2 * a + 1], c[2 + d])) for d in range(2)]
                    for d in range(2):
                        term = cadd(cmul_conj(b[0], q[2 * d]), cmul_conj(b[1], q[2 * d + 1]))
                        v = 2 * a + d
                        total[v] = term if total[v] is None else cadd(total[v], term)
            for v in range(4):
                model[turn, 0, v, time, lane] = total[v][0]
                model[turn, 1, v, time, lane] = total[v][1]
            return carry

        lax.fori_loop(0, blocks * halves, model_body, 0)

        other = 1 - own
        hop = send_d(turn, 0, model.at[turn, other], got_a.at[turn], 0)
        if turn > 0:
            pump(turn - 1, 1)

        jp = [(end(v, first), end(4 + v, first)) for v in range(4)]
        jq = [(end(v, second), end(4 + v, second)) for v in range(4)]

        def gram_of(j):
            m00 = re_mul(j[0], conj(j[0])) + re_mul(j[2], conj(j[2]))
            m11 = re_mul(j[1], conj(j[1])) + re_mul(j[3], conj(j[3]))
            m01 = cadd(cmul_conj(j[1], j[0]), cmul_conj(j[3], j[2]))
            return m00, m11, m01

        m00, m11, m01 = gram_of(jq)
        p00, p11, p01 = gram_of(jp)
        n1_00 = m00 * gram(0, 0) + m11 * gram(1, 1) + 2.0 * re_mul(m01, gram(0, 1))
        n1_11 = m00 * gram(2, 2) + m11 * gram(3, 3) + 2.0 * re_mul(m01, gram(2, 3))
        n1_01 = cadd(
            cadd(scale(m00, gram(0, 2)), scale(m11, gram(1, 3))),
            cadd(cmul(m01, gram(0, 3)), cmul(conj(m01), gram(1, 2))),
        )
        n2_00 = p00 * gram(0, 0) + p11 * gram(2, 2) + 2.0 * re_mul(p01, gram(2, 0))
        n2_11 = p00 * gram(1, 1) + p11 * gram(3, 3) + 2.0 * re_mul(p01, gram(3, 1))
        n2_01 = cadd(
            cadd(scale(p00, gram(1, 0)), scale(p11, gram(3, 2))),
            cadd(cmul(p01, gram(3, 0)), cmul(conj(p01), gram(1, 2))),
        )
        for n, (left, right) in enumerate(
            ((n1_00, n2_00), (n1_11, n2_11), (n1_01[0], n2_01[0]), (n1_01[1], n2_01[1]))
        ):
            vals_n[n * dirs : (n + 1) * dirs, first] = left
            vals_n[n * dirs : (n + 1) * dirs, second] = right

        hop.wait_recv()
        sum_a[turn, 0] = model[turn, own] + got_a[turn]
        for stage in range(1, stages):
            hop = send_d(turn, stage, sum_a.at[turn, stage - 1], got_b.at[turn, stage - 1], stage)
            if stage == 1:
                split_store(lhs_n, 4 * dirs, vals_n[...])
                found = join(jnp.dot(lhs_n[...], scatter_hot[...], preferred_element_type=f32), 4 * dirs)
                for g in range(4 * dirs // SUB):
                    for j in range(per):
                        seg_n[pl.ds(g * SUB * per + j, SUB, stride=per), :] = found[
                            g * SUB : (g + 1) * SUB, j * LANES : (j + 1) * LANES
                        ]
                if turn == 0:
                    start_consensus()
                    solve_weights()
                else:
                    for s in range(2, (ahead + 2) // 2):
                        pump(turn - 1, s)
            hop.wait_recv()
            target = sum_a.at[turn, stage] if stage + 1 < stages else sum_b.at[turn]
            target[...] = sum_a[turn, stage - 1] + got_b[turn, stage - 1]
        hop = send_d(turn, stages, sum_b.at[turn], got_c.at[turn], 0)
        if turn > 0:
            for s in range(max(2, (ahead + 2) // 2), ahead):
                pump(turn - 1, s)
        res[own] = vis[own] - sum_b[turn]
        hop.wait_recv()
        res[other] = vis[other] - got_c[turn]

        def cross_body(j, carry):
            lane = pl.ds(pl.multiple_of(j * LANES, LANES), LANES)
            r = [[res[v // 4, v % 4, h * SUB : (h + 1) * SUB, lane] for h in range(halves)] for v in range(8)]
            for k in range(dirs):
                c = [[coh[k, v, h * SUB : (h + 1) * SUB, lane] for h in range(halves)] for v in range(8)]
                for a in range(4):
                    for b in range(4):
                        real = sum(r[a][h] * c[b][h] + r[4 + a][h] * c[4 + b][h] for h in range(halves))
                        imag = sum(r[4 + a][h] * c[b][h] - r[a][h] * c[4 + b][h] for h in range(halves))
                        n = 2 * (4 * a + b)
                        cross[n * dirs + k : n * dirs + k + 1, lane] = jnp.sum(real, axis=0, keepdims=True)
                        cross[(n + 1) * dirs + k : (n + 1) * dirs + k + 1, lane] = jnp.sum(
                            imag, axis=0, keepdims=True
                        )
            return carry

        lax.fori_loop(0, blocks, cross_body, 0)

        def crossed(a, b):
            n = 2 * (4 * a + b)
            return (
                cross[n * dirs : (n + 1) * dirs, :],
                cross[(n + 1) * dirs : (n + 2) * dirs, :],
            )

        def herm(which):
            zero = [vals_n[n * dirs : (n + 1) * dirs, which] for n in range(4)]
            return zero[0], zero[1], (zero[2], zero[3])

        for which, j, other_end in ((first, jq, jp), (second, jp, jq)):
            h00, h11, h01 = herm(which)
            for a in range(2):
                for c in range(2):
                    total = None
                    for b in range(2):
                        for d in range(2):
                            if which is first:
                                term = cmul(j[2 * b + d], crossed(2 * a + b, 2 * c + d))
                            else:
                                term = cmul_conj(j[2 * b + d], crossed(2 * b + a, 2 * d + c))
                            total = term if total is None else cadd(total, term)
                    if c == 0:
                        extra = cadd(scale(h00, other_end[2 * a]), cmul_conj(other_end[2 * a + 1], h01))
                    else:
                        extra = cadd(cmul(other_end[2 * a], h01), scale(h11, other_end[2 * a + 1]))
                    total = cadd(total, extra)
                    for part in range(2):
                        n = 4 * part + 2 * a + c
                        vals[n * dirs : (n + 1) * dirs, which] = total[part]

        split_store(lhs, nrow, vals[...])
        found = join(jnp.dot(lhs[...], scatter_hot[...], preferred_element_type=f32), nrow)
        for g in range(nrow // SUB):
            for j in range(per):
                seg[pl.ds(g * SUB * per + j, SUB, stride=per), :] = found[
                    g * SUB : (g + 1) * SUB, j * LANES : (j + 1) * LANES
                ]

        def join_bands(previous):
            pump(previous, ahead)
            for k in range(dirs):
                for v in range(8):
                    here = pl.ds((v * dirs + k) * per, per)
                    total = None
                    for s in range(n_band):
                        term = weights[source(s)] * xall[previous, k, s, v]
                        total = term if total is None else total + term
                    cons[here, :] = total
                    fresh = dual[here, :] + RHO * (jones[here, :] - total)
                    if previous + 1 < ITERS:
                        dual[here, :] = fresh
                    else:
                        dual_out[halves_of(k, v)] = fresh

        if turn > 0:
            join_bands(turn - 1)

        for k in range(dirs):
            def rows_of(v):
                return pl.ds((v * dirs + k) * per, per)

            y = []
            for v in range(8):
                here = rows_of(v)
                y.append(seg[here, :] + RHO * cons[here, :] - dual[here, :])
            h00, h11, re01, im01 = [seg_n[rows_of(n), :] for n in range(4)]
            h00 = h00 + RHO
            h11 = h11 + RHO
            inverse = 1.0 / (h00 * h11 - (re01 * re01 + im01 * im01))
            h00, h11, h01 = h00 * inverse, h11 * inverse, (re01 * inverse, im01 * inverse)
            for a in range(2):
                y0, y1 = (y[2 * a], y[4 + 2 * a]), (y[2 * a + 1], y[4 + 2 * a + 1])
                minus0, minus1 = cmul_conj(y1, h01), cmul(y0, h01)
                for part in range(2):
                    for c in range(2):
                        if c == 0:
                            value = h11 * y0[part] - minus0[part]
                        else:
                            value = h00 * y1[part] - minus1[part]
                        v = 4 * part + 2 * a + c
                        here = rows_of(v)
                        jones[here, :] = value
                        if turn + 1 == ITERS:
                            jones_out[halves_of(k, v)] = value
                        xall[turn, k, 0, v] = value + dual[here, :] * (1.0 / RHO)
            for way, reach in enumerate((ahead, behind)):
                if reach:
                    send_x(turn, k, way, 0)

    last = ITERS - 1
    for s in range(1, ahead):
        pump(last, s)
    join_bands(last)

    def coeff_body(m, carry):
        for k in range(dirs):
            total = [None] * 8
            for s in range(n_band):
                factor = jnp.broadcast_to(gweights[source(s), pl.ds(m, 1), :], (SUB, LANES))
                for v in range(8):
                    term = factor * xall[last, k, s, v]
                    total[v] = term if total[v] is None else total[v] + term
            for v in range(8):
                coeffs[(m,) + halves_of(k, v)] = total[v]
        return carry

    lax.fori_loop(0, SUB, coeff_body, 0)

    for copies in x_copies:
        for copy in copies.values():
            copy.wait_send()
    for copy in d_copies:
        copy.wait_send()


def local(n_band, n_dir, vis, coh, jones_start, dual_start, consensus_start, freq_basis, pairs):
    f32 = jnp.float32
    dirs, times, base = coh.shape[1], coh.shape[-2], coh.shape[-1]
    stations = jones_start.shape[-1]
    per = stations // LANES
    nrow = 8 * dirs
    terms = freq_basis.shape[1]

    def enter(value):
        lead = value.shape[:-2]
        value = value.reshape(lead + (2, per, LANES))
        return jnp.swapaxes(value, -2, -3).reshape(lead + (2 * per, LANES))

    def leave(value, shape):
        value = value.reshape(value.shape[:-2] + (per, 2, LANES))
        return jnp.swapaxes(value, -2, -3).reshape(shape)

    stages = n_dir.bit_length() - 1
    half = (4, times, base)
    vmem = pl.BlockSpec(memory_space=pltpu.VMEM)
    far = pl.BlockSpec(memory_space=pl.ANY)
    raw = (dirs, 4, 2 * per, LANES)
    raw_out = jax.ShapeDtypeStruct(raw, f32)
    bf16 = jnp.bfloat16
    jones, dual, coeffs = pl.pallas_call(
        functools.partial(kernel, n_band, n_dir, dirs, times, base, stations),
        out_shape=(raw_out, raw_out, jax.ShapeDtypeStruct((terms,) + raw, f32)),
        in_specs=[far, far, vmem, vmem, far, pl.BlockSpec(memory_space=pltpu.SMEM), vmem],
        out_specs=(vmem,) * 3,
        scratch_shapes=[
            pltpu.VMEM((2,) + half, f32),
            pltpu.VMEM((dirs, 8, times, base), f32),
            pltpu.VMEM((terms,) + raw, f32),
            pltpu.VMEM((nrow * per, LANES), f32),
            pltpu.VMEM((nrow * per, LANES), f32),
            pltpu.VMEM((SUB, LANES), f32),
            pltpu.VMEM((2 * base, LANES), jnp.int32),
            pltpu.VMEM((nrow * per, LANES), f32),
            pltpu.VMEM((ITERS, dirs, n_band, 8, per, LANES), f32),
            pltpu.VMEM((n_band, SUB, LANES), f32),
            pltpu.VMEM((n_band, SUB, LANES), f32),
            pltpu.VMEM((n_band, SUB, LANES), f32),
            pltpu.VMEM((stations, 2 * base), bf16),
            pltpu.VMEM((2 * base, stations), bf16),
            pltpu.VMEM((PIECES * nrow, max(stations, 2 * base)), bf16),
            pltpu.VMEM((PIECES * 4 * dirs, 2 * base), bf16),
            pltpu.VMEM((nrow, 2 * base), f32),
            pltpu.VMEM((20 * dirs, base), f32),
            pltpu.VMEM((32 * dirs, base), f32),
            pltpu.VMEM((nrow, 2 * base), f32),
            pltpu.VMEM((4 * dirs, 2 * base), f32),
            pltpu.VMEM((nrow * per, LANES), f32),
            pltpu.VMEM((4 * dirs * per, LANES), f32),
            pltpu.VMEM((ITERS, 2) + half, f32),
            pltpu.VMEM((ITERS,) + half, f32),
            pltpu.VMEM((ITERS, stages - 1) + half, f32),
            pltpu.VMEM((ITERS, stages - 1) + half, f32),
            pltpu.VMEM((ITERS,) + half, f32),
            pltpu.VMEM((ITERS,) + half, f32),
            pltpu.VMEM((2,) + half, f32),
            pltpu.SemaphoreType.DMA((3,)),
            pltpu.SemaphoreType.DMA((n_band,)),
            pltpu.SemaphoreType.DMA((n_band,)),
            pltpu.SemaphoreType.DMA((ITERS, dirs, n_band - 1)),
            pltpu.SemaphoreType.DMA((ITERS, dirs, n_band - 1)),
            pltpu.SemaphoreType.DMA((ITERS, stages + 1)),
            pltpu.SemaphoreType.DMA((ITERS, stages + 1)),
        ],
        compiler_params=pltpu.CompilerParams(
            collective_id=0, has_side_effects=True, vmem_limit_bytes=60 * 1024 * 1024
        ),
    )(
        vis.reshape((2,) + half),
        coh.reshape(dirs, 8, times, base),
        enter(jones_start.reshape((dirs, 4, 2, stations))),
        enter(dual_start.reshape((dirs, 4, 2, stations))),
        enter(consensus_start.reshape((terms, dirs, 4, 2, stations))),
        freq_basis,
        pairs,
    )
    return (
        leave(jones, jones_start.shape),
        leave(dual, jones_start.shape),
        leave(coeffs, consensus_start.shape),
    )


def solution(mesh):
    in_specs = (
        P("band", None, None, None, None, None),
        P("band", "dir", None, None, None, None, None),
        P("band", "dir", None, None, None, None),
        P("band", "dir", None, None, None, None),
        P(None, "dir", None, None, None, None),
        P("band", None),
        P(),
    )
    out_specs = (
        P("band", "dir", None, None, None, None),
        P("band", "dir", None, None, None, None),
        P(None, "dir", None, None, None, None),
    )
    body = functools.partial(local, mesh.shape["band"], mesh.shape["dir"])
    return jax.shard_map(body, mesh=mesh, in_specs=in_specs, out_specs=out_specs, check_vma=False)
```

```python
import functools

import jax
import jax.numpy as jnp
from jax import lax
from jax.experimental import pallas as pl
from jax.experimental.pallas import tpu as pltpu
from jax.sharding import PartitionSpec as P

ITERS = 3
RHO = 5.0
RIDGE = 0.25
LANES = 128
SUB = 8
PIECES = 3
MESH = pl.DeviceIdType.MESH


def cmul(a, b):
    return (a[0] * b[0] - a[1] * b[1], a[0] * b[1] + a[1] * b[0])


def cmul_conj(a, b):
    return (a[0] * b[0] + a[1] * b[1], a[1] * b[0] - a[0] * b[1])


def cadd(a, b):
    return (a[0] + b[0], a[1] + b[1])


def conj(a):
    return (a[0], -a[1])


def re_mul(a, b):
    return a[0] * b[0] - a[1] * b[1]


def scale(r, a):
    return (r * a[0], r * a[1])


def split_store(ref, rows, value):
    left = value
    for piece in range(PIECES):
        part = left.astype(jnp.bfloat16)
        ref[piece * rows : (piece + 1) * rows, :] = part
        if piece + 1 < PIECES:
            left = left - part.astype(jnp.float32)


def join(value, rows):
    total = value[0:rows]
    for piece in range(1, PIECES):
        total = total + value[piece * rows : (piece + 1) * rows]
    return total


def kernel(
    n_band, n_dir, dirs, times, base, stations,
    vis_far, coh_far, jones0, dual0, coeffs0_far, basis, pairs_ref,
    jones_out, dual_out, coeffs,
    vis, coh, coeffs0, jones, dual, row, ids_col,
    cons, xall, rows_all, weights, gweights,
    gather_hot, scatter_hot, lhs, lhs_n, ends, grams, cross, vals, vals_n, seg, seg_n,
    model, got_a, sum_a, got_b, sum_b, got_c, res,
    load_sem, row_send, row_recv, x_send, x_recv, d_send, d_recv,
):
    f32 = jnp.float32
    nrow = 8 * dirs
    per = stations // LANES
    me = lax.axis_index("band")
    mine = lax.axis_index("dir")
    blocks = base // LANES
    halves = times // SUB
    stages = n_dir.bit_length() - 1

    def at(pos):
        half = pos // (n_band // 2)
        return (1 - half) * (2 * pos) + half * (2 * (n_band - 1 - pos) + 1)

    odd = lax.rem(me, 2)
    pos = (1 - odd) * (me // 2) + odd * (n_band - 1 - me // 2)
    nexts = (at(lax.rem(pos + 1, n_band)), at(lax.rem(pos + n_band - 1, n_band)))

    def flip(stage):
        bit = lax.rem(mine // (1 << stage), 2)
        return mine + (1 - 2 * bit) * (1 << stage)

    own = lax.rem(mine, 2)

    loads = []
    for n, (far, near) in enumerate(((coh_far, coh), (vis_far, vis), (coeffs0_far, coeffs0))):
        loads.append(pltpu.make_async_copy(far, near, load_sem.at[n]))
        loads[-1].start()

    barrier = pltpu.get_barrier_semaphore()
    for step in range(1, n_band):
        pl.semaphore_signal(
            barrier, inc=1, device_id={"band": lax.rem(me + step, n_band)}, device_id_type=MESH
        )
    for stage in range(stages):
        pl.semaphore_signal(barrier, inc=1, device_id={"dir": flip(stage)}, device_id_type=MESH)

    def halves_of(k, v):
        return (k, v // 2, pl.ds(v % 2, per, stride=2), slice(None))

    def packed(k, v):
        return pl.ds((v * dirs + k) * per, per)

    row[...] = jnp.zeros((SUB, LANES), f32)
    for m in range(SUB):
        row[m : m + 1, :] = jnp.full((1, LANES), basis[0, m], f32)
    for k in range(dirs):
        for v in range(8):
            jones[packed(k, v), :] = jones0[halves_of(k, v)]
            dual[packed(k, v), :] = dual0[halves_of(k, v)]

    for j in range(2 * base // LANES):
        lane = (j * LANES) % base
        which = (j * LANES) // base
        ids = jnp.broadcast_to(pairs_ref[which : which + 1, lane : lane + LANES], (LANES, LANES))
        ids_col[j * LANES : (j + 1) * LANES, :] = jnp.transpose(ids)
    step_rows = 32

    def hot_body(i, carry):
        start = pl.multiple_of(i * step_rows, step_rows)
        for j in range(2 * base // LANES):
            lane = slice(j * LANES, (j + 1) * LANES)
            sid = lax.broadcasted_iota(jnp.int32, (step_rows, LANES), 0) + i * step_rows
            which, low = (j * LANES) // base, (j * LANES) % base
            ids = pairs_ref[which : which + 1, low : low + LANES]
            same = sid == jnp.broadcast_to(ids, (step_rows, LANES))
            gather_hot[pl.ds(start, step_rows), lane] = jnp.where(same, 1.0, 0.0).astype(jnp.bfloat16)
        return carry

    lax.fori_loop(0, stations // step_rows, hot_body, 0)

    def hot_body2(i, carry):
        start = pl.multiple_of(i * step_rows, step_rows)
        col = ids_col[pl.ds(start, step_rows), :]
        for j in range(stations // LANES):
            lane = slice(j * LANES, (j + 1) * LANES)
            sid = lax.broadcasted_iota(jnp.int32, (step_rows, LANES), 1) + j * LANES
            scatter_hot[pl.ds(start, step_rows), lane] = jnp.where(sid == col, 1.0, 0.0).astype(jnp.bfloat16)
        return carry

    lax.fori_loop(0, 2 * base // step_rows, hot_body2, 0)

    pl.semaphore_wait(barrier, n_band - 1 + stages)

    row_copies = []
    for step in range(1, n_band):
        copy = pltpu.make_async_remote_copy(
            src_ref=row,
            dst_ref=rows_all.at[step],
            send_sem=row_send.at[step],
            recv_sem=row_recv.at[step],
            device_id={"band": lax.rem(me + step, n_band)},
            device_id_type=MESH,
        )
        copy.start()
        row_copies.append(copy)

    loads[0].wait()

    pairs = [(a, b) for a in range(4) for b in range(a, 4)]

    def gram_body(j, carry):
        lane = pl.ds(pl.multiple_of(j * LANES, LANES), LANES)
        for k in range(dirs):
            c = [
                [coh[k, v, h * SUB : (h + 1) * SUB, lane] for h in range(halves)]
                for v in range(8)
            ]
            for n, (a, b) in enumerate(pairs):
                real = sum(c[a][h] * c[b][h] + c[4 + a][h] * c[4 + b][h] for h in range(halves))
                grams[(2 * n) * dirs + k : (2 * n) * dirs + k + 1, lane] = jnp.sum(real, axis=0, keepdims=True)
                if a != b:
                    imag = sum(c[4 + a][h] * c[b][h] - c[a][h] * c[4 + b][h] for h in range(halves))
                    grams[(2 * n + 1) * dirs + k : (2 * n + 1) * dirs + k + 1, lane] = jnp.sum(
                        imag, axis=0, keepdims=True
                    )
        return carry

    lax.fori_loop(0, blocks, gram_body, 0)

    def gram(a, b):
        if a > b:
            return conj(gram(b, a))
        n = pairs.index((a, b))
        real = grams[(2 * n) * dirs : (2 * n + 1) * dirs, :]
        if a == b:
            return real
        return (real, grams[(2 * n + 1) * dirs : (2 * n + 2) * dirs, :])

    def start_consensus():
        loads[1].wait()
        loads[2].wait()
        for k in range(dirs):
            for v in range(8):
                total = basis[0, 0] * coeffs0[(0,) + halves_of(k, v)]
                for m in range(1, SUB):
                    total = total + basis[0, m] * coeffs0[(m,) + halves_of(k, v)]
                cons[packed(k, v), :] = total

    def solve_weights():
        for copy in row_copies:
            copy.wait()
        rows_all[0] = row[...]
        held = [rows_all[s] for s in range(n_band)]
        columns = []
        for m in range(SUB):
            total = held[0] * held[0][m : m + 1, :]
            for s in range(1, n_band):
                total = total + held[s] * held[s][m : m + 1, :]
            ident = jnp.where(lax.broadcasted_iota(jnp.int32, (SUB, LANES), 0) == m, RIDGE * n_band, 0.0)
            columns.append(total + ident.astype(f32))
        right = list(held)
        iota = lax.broadcasted_iota(jnp.int32, (SUB, LANES), 0)
        for i in range(SUB):
            inverse = 1.0 / columns[i][i : i + 1, :]
            factor = columns[i]
            for group in (columns, right):
                for c in range(len(group)):
                    lead = jnp.broadcast_to(group[c][i : i + 1, :] * inverse, (SUB, LANES))
                    group[c] = jnp.where(iota == i, lead, group[c] - factor * lead)
        for s in range(n_band):
            band = lax.rem(me + n_band - s, n_band)
            gweights[band] = right[s]
            weights[band] = jnp.broadcast_to(
                jnp.sum(right[s] * held[0], axis=0, keepdims=True), (SUB, LANES)
            )

    x_copies = [{} for _ in range(ITERS)]

    ahead = n_band // 2
    behind = n_band - 1 - ahead

    def slot_of(way, distance):
        if distance > behind:
            return n_band - 1
        return distance + way * behind if distance else 0

    def reach_of(k, way):
        return ahead if way == k % 2 else behind

    def send_x(turn, k, way, distance):
        to = slot_of(way, distance + 1)
        copy = pltpu.make_async_remote_copy(
            src_ref=xall.at[turn, k, slot_of(way, distance)],
            dst_ref=xall.at[turn, k, to],
            send_sem=x_send.at[turn, k, to - 1],
            recv_sem=x_recv.at[turn, k, to - 1],
            device_id={"band": nexts[way]},
            device_id_type=MESH,
        )
        copy.start()
        x_copies[turn][(k, way, distance + 1)] = copy

    def pump(turn, distance, chosen=range(dirs)):
        for k in chosen:
            for way in range(2):
                reach = reach_of(k, way)
                if distance <= reach:
                    x_copies[turn][(k, way, distance)].wait_recv()
                    if distance < reach:
                        send_x(turn, k, way, distance)

    def source(slot):
        if slot <= behind:
            return at(lax.rem(pos + n_band - slot, n_band))
        return at(lax.rem(pos + slot - behind, n_band))

    def end(comp, lane):
        return ends[comp * dirs : (comp + 1) * dirs, lane]

    early, late = range(dirs // 2), range(dirs // 2, dirs)
    d_copies = []

    def send_d(turn, n, src, dst, stage):
        copy = pltpu.make_async_remote_copy(
            src_ref=src,
            dst_ref=dst,
            send_sem=d_send.at[turn, n],
            recv_sem=d_recv.at[turn, n],
            device_id={"dir": flip(stage)},
            device_id_type=MESH,
        )
        copy.start()
        d_copies.append(copy)
        return copy

    first = slice(0, base)
    second = slice(base, 2 * base)

    for turn in range(ITERS):
        for g in range(nrow // SUB):
            for j in range(per):
                value = jones[pl.ds(g * SUB * per + j, SUB, stride=per), :]
                left = value
                for piece in range(PIECES):
                    part = left.astype(jnp.bfloat16)
                    lhs[
                        piece * nrow + g * SUB : piece * nrow + (g + 1) * SUB,
                        j * LANES : (j + 1) * LANES,
                    ] = part
                    left = left - part.astype(f32)
        ends[...] = join(jnp.dot(lhs[...], gather_hot[...], preferred_element_type=f32), nrow)

        def model_body(i, carry):
            j = i // halves
            h = lax.rem(i, halves)
            lane = pl.ds(pl.multiple_of(j * LANES, LANES), LANES)
            lane_q = pl.ds(pl.multiple_of(base + j * LANES, LANES), LANES)
            time = pl.ds(pl.multiple_of(h * SUB, SUB), SUB)
            total = [None] * 4
            for k in range(dirs):
                c = [(coh[k, v, time, lane], coh[k, 4 + v, time, lane]) for v in range(4)]

                def spread(v, where):
                    return tuple(
                        jnp.broadcast_to(
                            ends[(4 * part + v) * dirs + k : (4 * part + v) * dirs + k + 1, where],
                            (SUB, LANES),
                        )
                        for part in range(2)
                    )

                p = [spread(v, lane) for v in range(4)]
                q = [spread(v, lane_q) for v in range(4)]
                for a in range(2):
                    b = [cadd(cmul(p[2 * a], c[d]), cmul(p[2 * a + 1], c[2 + d])) for d in range(2)]
                    for d in range(2):
                        term = cadd(cmul_conj(b[0], q[2 * d]), cmul_conj(b[1], q[2 * d + 1]))
                        v = 2 * a + d
                        total[v] = term if total[v] is None else cadd(total[v], term)
            for v in range(4):
                model[turn, 0, v, time, lane] = total[v][0]
                model[turn, 1, v, time, lane] = total[v][1]
            return carry

        lax.fori_loop(0, blocks * halves, model_body, 0)

        other = 1 - own
        hop = send_d(turn, 0, model.at[turn, other], got_a.at[turn], 0)
        if turn > 0:
            pump(turn - 1, 1, early)

        jp = [(end(v, first), end(4 + v, first)) for v in range(4)]
        jq = [(end(v, second), end(4 + v, second)) for v in range(4)]

        def gram_of(j):
            m00 = re_mul(j[0], conj(j[0])) + re_mul(j[2], conj(j[2]))
            m11 = re_mul(j[1], conj(j[1])) + re_mul(j[3], conj(j[3]))
            m01 = cadd(cmul_conj(j[1], j[0]), cmul_conj(j[3], j[2]))
            return m00, m11, m01

        m00, m11, m01 = gram_of(jq)
        p00, p11, p01 = gram_of(jp)
        n1_00 = m00 * gram(0, 0) + m11 * gram(1, 1) + 2.0 * re_mul(m01, gram(0, 1))
        n1_11 = m00 * gram(2, 2) + m11 * gram(3, 3) + 2.0 * re_mul(m01, gram(2, 3))
        n1_01 = cadd(
            cadd(scale(m00, gram(0, 2)), scale(m11, gram(1, 3))),
            cadd(cmul(m01, gram(0, 3)), cmul(conj(m01), gram(1, 2))),
        )
        n2_00 = p00 * gram(0, 0) + p11 * gram(2, 2) + 2.0 * re_mul(p01, gram(2, 0))
        n2_11 = p00 * gram(1, 1) + p11 * gram(3, 3) + 2.0 * re_mul(p01, gram(3, 1))
        n2_01 = cadd(
            cadd(scale(p00, gram(1, 0)), scale(p11, gram(3, 2))),
            cadd(cmul(p01, gram(3, 0)), cmul(conj(p01), gram(1, 2))),
        )
        for n, (left, right) in enumerate(
            ((n1_00, n2_00), (n1_11, n2_11), (n1_01[0], n2_01[0]), (n1_01[1], n2_01[1]))
        ):
            vals_n[n * dirs : (n + 1) * dirs, first] = left
            vals_n[n * dirs : (n + 1) * dirs, second] = right

        hop.wait_recv()
        sum_a[turn, 0] = model[turn, own] + got_a[turn]
        for stage in range(1, stages):
            hop = send_d(turn, stage, sum_a.at[turn, stage - 1], got_b.at[turn, stage - 1], stage)
            if stage == 1:
                if turn > 0:
                    pump(turn - 1, 1, late)
                split_store(lhs_n, 4 * dirs, vals_n[...])
                found = join(jnp.dot(lhs_n[...], scatter_hot[...], preferred_element_type=f32), 4 * dirs)
                for g in range(4 * dirs // SUB):
                    for j in range(per):
                        seg_n[pl.ds(g * SUB * per + j, SUB, stride=per), :] = found[
                            g * SUB : (g + 1) * SUB, j * LANES : (j + 1) * LANES
                        ]
                if turn == 0:
                    start_consensus()
                    solve_weights()
                else:
                    for s in range(2, (ahead + 2) // 2):
                        pump(turn - 1, s)
            hop.wait_recv()
            target = sum_a.at[turn, stage] if stage + 1 < stages else sum_b.at[turn]
            target[...] = sum_a[turn, stage - 1] + got_b[turn, stage - 1]
        hop = send_d(turn, stages, sum_b.at[turn], got_c.at[turn], 0)
        if turn > 0:
            for s in range(max(2, (ahead + 2) // 2), ahead):
                pump(turn - 1, s, early if s + 1 == ahead else range(dirs))
        res[own] = vis[own] - sum_b[turn]
        hop.wait_recv()
        res[other] = vis[other] - got_c[turn]
        if turn > 0 and ahead - 1 >= max(2, (ahead + 2) // 2):
            pump(turn - 1, ahead - 1, late)

        def cross_body(j, carry):
            lane = pl.ds(pl.multiple_of(j * LANES, LANES), LANES)
            r = [[res[v // 4, v % 4, h * SUB : (h + 1) * SUB, lane] for h in range(halves)] for v in range(8)]
            for k in range(dirs):
                c = [[coh[k, v, h * SUB : (h + 1) * SUB, lane] for h in range(halves)] for v in range(8)]
                for a in range(4):
                    for b in range(4):
                        real = sum(r[a][h] * c[b][h] + r[4 + a][h] * c[4 + b][h] for h in range(halves))
                        imag = sum(r[4 + a][h] * c[b][h] - r[a][h] * c[4 + b][h] for h in range(halves))
                        n = 2 * (4 * a + b)
                        cross[n * dirs + k : n * dirs + k + 1, lane] = jnp.sum(real, axis=0, keepdims=True)
                        cross[(n + 1) * dirs + k : (n + 1) * dirs + k + 1, lane] = jnp.sum(
                            imag, axis=0, keepdims=True
                        )
            return carry

        lax.fori_loop(0, blocks, cross_body, 0)

        def crossed(a, b):
            n = 2 * (4 * a + b)
            return (
                cross[n * dirs : (n + 1) * dirs, :],
                cross[(n + 1) * dirs : (n + 2) * dirs, :],
            )

        def herm(which):
            zero = [vals_n[n * dirs : (n + 1) * dirs, which] for n in range(4)]
            return zero[0], zero[1], (zero[2], zero[3])

        for which, j, other_end in ((first, jq, jp), (second, jp, jq)):
            h00, h11, h01 = herm(which)
            for a in range(2):
                for c in range(2):
                    total = None
                    for b in range(2):
                        for d in range(2):
                            if which is first:
                                term = cmul(j[2 * b + d], crossed(2 * a + b, 2 * c + d))
                            else:
                                term = cmul_conj(j[2 * b + d], crossed(2 * b + a, 2 * d + c))
                            total = term if total is None else cadd(total, term)
                    if c == 0:
                        extra = cadd(scale(h00, other_end[2 * a]), cmul_conj(other_end[2 * a + 1], h01))
                    else:
                        extra = cadd(cmul(other_end[2 * a], h01), scale(h11, other_end[2 * a + 1]))
                    total = cadd(total, extra)
                    for part in range(2):
                        n = 4 * part + 2 * a + c
                        vals[n * dirs : (n + 1) * dirs, which] = total[part]

        split_store(lhs, nrow, vals[...])
        found = join(jnp.dot(lhs[...], scatter_hot[...], preferred_element_type=f32), nrow)
        for g in range(nrow // SUB):
            for j in range(per):
                seg[pl.ds(g * SUB * per + j, SUB, stride=per), :] = found[
                    g * SUB : (g + 1) * SUB, j * LANES : (j + 1) * LANES
                ]

        def join_bands(previous):
            pump(previous, ahead)
            for k in range(dirs):
                for v in range(8):
                    here = pl.ds((v * dirs + k) * per, per)
                    total = None
                    for s in range(n_band):
                        term = weights[source(s)] * xall[previous, k, s, v]
                        total = term if total is None else total + term
                    cons[here, :] = total
                    fresh = dual[here, :] + RHO * (jones[here, :] - total)
                    if previous + 1 < ITERS:
                        dual[here, :] = fresh
                    else:
                        dual_out[halves_of(k, v)] = fresh

        if turn > 0:
            join_bands(turn - 1)

        for k in range(dirs):
            def rows_of(v):
                return pl.ds((v * dirs + k) * per, per)

            y = []
            for v in range(8):
                here = rows_of(v)
                y.append(seg[here, :] + RHO * cons[here, :] - dual[here, :])
            h00, h11, re01, im01 = [seg_n[rows_of(n), :] for n in range(4)]
            h00 = h00 + RHO
            h11 = h11 + RHO
            inverse = 1.0 / (h00 * h11 - (re01 * re01 + im01 * im01))
            h00, h11, h01 = h00 * inverse, h11 * inverse, (re01 * inverse, im01 * inverse)
            for a in range(2):
                y0, y1 = (y[2 * a], y[4 + 2 * a]), (y[2 * a + 1], y[4 + 2 * a + 1])
                minus0, minus1 = cmul_conj(y1, h01), cmul(y0, h01)
                for part in range(2):
                    for c in range(2):
                        if c == 0:
                            value = h11 * y0[part] - minus0[part]
                        else:
                            value = h00 * y1[part] - minus1[part]
                        v = 4 * part + 2 * a + c
                        here = rows_of(v)
                        jones[here, :] = value
                        if turn + 1 == ITERS:
                            jones_out[halves_of(k, v)] = value
                        xall[turn, k, 0, v] = value + dual[here, :] * (1.0 / RHO)
            for way in range(2):
                if reach_of(k, way):
                    send_x(turn, k, way, 0)

    last = ITERS - 1
    for s in range(1, ahead):
        pump(last, s)
    join_bands(last)

    def coeff_body(m, carry):
        for k in range(dirs):
            total = [None] * 8
            for s in range(n_band):
                factor = jnp.broadcast_to(gweights[source(s), pl.ds(m, 1), :], (SUB, LANES))
                for v in range(8):
                    term = factor * xall[last, k, s, v]
                    total[v] = term if total[v] is None else total[v] + term
            for v in range(8):
                coeffs[(m,) + halves_of(k, v)] = total[v]
        return carry

    lax.fori_loop(0, SUB, coeff_body, 0)

    for copies in x_copies:
        for copy in copies.values():
            copy.wait_send()
    for copy in d_copies:
        copy.wait_send()


def local(n_band, n_dir, vis, coh, jones_start, dual_start, consensus_start, freq_basis, pairs):
    f32 = jnp.float32
    dirs, times, base = coh.shape[1], coh.shape[-2], coh.shape[-1]
    stations = jones_start.shape[-1]
    per = stations // LANES
    nrow = 8 * dirs
    terms = freq_basis.shape[1]

    def enter(value):
        lead = value.shape[:-2]
        value = value.reshape(lead + (2, per, LANES))
        return jnp.swapaxes(value, -2, -3).reshape(lead + (2 * per, LANES))

    def leave(value, shape):
        value = value.reshape(value.shape[:-2] + (per, 2, LANES))
        return jnp.swapaxes(value, -2, -3).reshape(shape)

    stages = n_dir.bit_length() - 1
    half = (4, times, base)
    vmem = pl.BlockSpec(memory_space=pltpu.VMEM)
    far = pl.BlockSpec(memory_space=pl.ANY)
    raw = (dirs, 4, 2 * per, LANES)
    raw_out = jax.ShapeDtypeStruct(raw, f32)
    bf16 = jnp.bfloat16
    jones, dual, coeffs = pl.pallas_call(
        functools.partial(kernel, n_band, n_dir, dirs, times, base, stations),
        out_shape=(raw_out, raw_out, jax.ShapeDtypeStruct((terms,) + raw, f32)),
        in_specs=[far, far, vmem, vmem, far, pl.BlockSpec(memory_space=pltpu.SMEM), vmem],
        out_specs=(vmem,) * 3,
        scratch_shapes=[
            pltpu.VMEM((2,) + half, f32),
            pltpu.VMEM((dirs, 8, times, base), f32),
            pltpu.VMEM((terms,) + raw, f32),
            pltpu.VMEM((nrow * per, LANES), f32),
            pltpu.VMEM((nrow * per, LANES), f32),
            pltpu.VMEM((SUB, LANES), f32),
            pltpu.VMEM((2 * base, LANES), jnp.int32),
            pltpu.VMEM((nrow * per, LANES), f32),
            pltpu.VMEM((ITERS, dirs, n_band, 8, per, LANES), f32),
            pltpu.VMEM((n_band, SUB, LANES), f32),
            pltpu.VMEM((n_band, SUB, LANES), f32),
            pltpu.VMEM((n_band, SUB, LANES), f32),
            pltpu.VMEM((stations, 2 * base), bf16),
            pltpu.VMEM((2 * base, stations), bf16),
            pltpu.VMEM((PIECES * nrow, max(stations, 2 * base)), bf16),
            pltpu.VMEM((PIECES * 4 * dirs, 2 * base), bf16),
            pltpu.VMEM((nrow, 2 * base), f32),
            pltpu.VMEM((20 * dirs, base), f32),
            pltpu.VMEM((32 * dirs, base), f32),
            pltpu.VMEM((nrow, 2 * base), f32),
            pltpu.VMEM((4 * dirs, 2 * base), f32),
            pltpu.VMEM((nrow * per, LANES), f32),
            pltpu.VMEM((4 * dirs * per, LANES), f32),
            pltpu.VMEM((ITERS, 2) + half, f32),
            pltpu.VMEM((ITERS,) + half, f32),
            pltpu.VMEM((ITERS, stages - 1) + half, f32),
            pltpu.VMEM((ITERS, stages - 1) + half, f32),
            pltpu.VMEM((ITERS,) + half, f32),
            pltpu.VMEM((ITERS,) + half, f32),
            pltpu.VMEM((2,) + half, f32),
            pltpu.SemaphoreType.DMA((3,)),
            pltpu.SemaphoreType.DMA((n_band,)),
            pltpu.SemaphoreType.DMA((n_band,)),
            pltpu.SemaphoreType.DMA((ITERS, dirs, n_band - 1)),
            pltpu.SemaphoreType.DMA((ITERS, dirs, n_band - 1)),
            pltpu.SemaphoreType.DMA((ITERS, stages + 1)),
            pltpu.SemaphoreType.DMA((ITERS, stages + 1)),
        ],
        compiler_params=pltpu.CompilerParams(
            collective_id=0, has_side_effects=True, vmem_limit_bytes=60 * 1024 * 1024
        ),
    )(
        vis.reshape((2,) + half),
        coh.reshape(dirs, 8, times, base),
        enter(jones_start.reshape((dirs, 4, 2, stations))),
        enter(dual_start.reshape((dirs, 4, 2, stations))),
        enter(consensus_start.reshape((terms, dirs, 4, 2, stations))),
        freq_basis,
        pairs,
    )
    return (
        leave(jones, jones_start.shape),
        leave(dual, jones_start.shape),
        leave(coeffs, consensus_start.shape),
    )


def solution(mesh):
    in_specs = (
        P("band", None, None, None, None, None),
        P("band", "dir", None, None, None, None, None),
        P("band", "dir", None, None, None, None),
        P("band", "dir", None, None, None, None),
        P(None, "dir", None, None, None, None),
        P("band", None),
        P(),
    )
    out_specs = (
        P("band", "dir", None, None, None, None),
        P("band", "dir", None, None, None, None),
        P(None, "dir", None, None, None, None),
    )
    body = functools.partial(local, mesh.shape["band"], mesh.shape["dir"])
    return jax.shard_map(body, mesh=mesh, in_specs=in_specs, out_specs=out_specs, check_vma=False)
```

```python
import functools

import jax
import jax.numpy as jnp
from jax import lax
from jax.experimental import pallas as pl
from jax.experimental.pallas import tpu as pltpu
from jax.sharding import PartitionSpec as P

ITERS = 3
RHO = 5.0
RIDGE = 0.25
LANES = 128
SUB = 8
PIECES = 3
MESH = pl.DeviceIdType.MESH


def cmul(a, b):
    return (a[0] * b[0] - a[1] * b[1], a[0] * b[1] + a[1] * b[0])


def cmul_conj(a, b):
    return (a[0] * b[0] + a[1] * b[1], a[1] * b[0] - a[0] * b[1])


def cadd(a, b):
    return (a[0] + b[0], a[1] + b[1])


def conj(a):
    return (a[0], -a[1])


def re_mul(a, b):
    return a[0] * b[0] - a[1] * b[1]


def scale(r, a):
    return (r * a[0], r * a[1])


def split_store(ref, rows, value):
    left = value
    for piece in range(PIECES):
        part = left.astype(jnp.bfloat16)
        ref[piece * rows : (piece + 1) * rows, :] = part
        if piece + 1 < PIECES:
            left = left - part.astype(jnp.float32)


def join(value, rows):
    total = value[0:rows]
    for piece in range(1, PIECES):
        total = total + value[piece * rows : (piece + 1) * rows]
    return total


def kernel(
    n_band, n_dir, dirs, times, base, stations,
    vis_far, coh_far, jones0, dual0, coeffs0_far, basis, pairs_ref,
    jones_out, dual_out, coeffs,
    vis, coh, coeffs0, jones, dual, row, ids_col,
    cons, xall, rows_all, weights, gweights,
    gather_hot, scatter_hot, lhs, lhs_n, ends, grams, cross, vals, vals_n, seg, seg_n,
    model, got_a, sum_a, got_b, sum_b, got_c, res,
    load_sem, row_send, row_recv, x_send, x_recv, d_send, d_recv,
):
    f32 = jnp.float32
    nrow = 8 * dirs
    per = stations // LANES
    me = lax.axis_index("band")
    mine = lax.axis_index("dir")
    blocks = base // LANES
    halves = times // SUB
    stages = n_dir.bit_length() - 1

    def at(pos):
        half = pos // (n_band // 2)
        return (1 - half) * (2 * pos) + half * (2 * (n_band - 1 - pos) + 1)

    odd = lax.rem(me, 2)
    pos = (1 - odd) * (me // 2) + odd * (n_band - 1 - me // 2)
    nexts = (at(lax.rem(pos + 1, n_band)), at(lax.rem(pos + n_band - 1, n_band)))

    def flip(stage):
        bit = lax.rem(mine // (1 << stage), 2)
        return mine + (1 - 2 * bit) * (1 << stage)

    own = lax.rem(mine, 2)

    loads = []
    for n, (far, near) in enumerate(((coh_far, coh), (vis_far, vis), (coeffs0_far, coeffs0))):
        loads.append(pltpu.make_async_copy(far, near, load_sem.at[n]))
        loads[-1].start()

    barrier = pltpu.get_barrier_semaphore()
    for step in range(1, n_band):
        pl.semaphore_signal(
            barrier, inc=1, device_id={"band": lax.rem(me + step, n_band)}, device_id_type=MESH
        )
    for stage in range(stages):
        pl.semaphore_signal(barrier, inc=1, device_id={"dir": flip(stage)}, device_id_type=MESH)

    def halves_of(k, v):
        return (k, v // 2, pl.ds(v % 2, per, stride=2), slice(None))

    def packed(k, v):
        return pl.ds((v * dirs + k) * per, per)

    row[...] = jnp.zeros((SUB, LANES), f32)
    for m in range(SUB):
        row[m : m + 1, :] = jnp.full((1, LANES), basis[0, m], f32)
    for k in range(dirs):
        for v in range(8):
            jones[packed(k, v), :] = jones0[halves_of(k, v)]
            dual[packed(k, v), :] = dual0[halves_of(k, v)]

    for j in range(2 * base // LANES):
        lane = (j * LANES) % base
        which = (j * LANES) // base
        ids = jnp.broadcast_to(pairs_ref[which : which + 1, lane : lane + LANES], (LANES, LANES))
        ids_col[j * LANES : (j + 1) * LANES, :] = jnp.transpose(ids)
    step_rows = 32

    def hot_body(i, carry):
        start = pl.multiple_of(i * step_rows, step_rows)
        for j in range(2 * base // LANES):
            lane = slice(j * LANES, (j + 1) * LANES)
            sid = lax.broadcasted_iota(jnp.int32, (step_rows, LANES), 0) + i * step_rows
            which, low = (j * LANES) // base, (j * LANES) % base
            ids = pairs_ref[which : which + 1, low : low + LANES]
            same = sid == jnp.broadcast_to(ids, (step_rows, LANES))
            gather_hot[pl.ds(start, step_rows), lane] = jnp.where(same, 1.0, 0.0).astype(jnp.bfloat16)
        return carry

    lax.fori_loop(0, stations // step_rows, hot_body, 0)

    def hot_body2(i, carry):
        start = pl.multiple_of(i * step_rows, step_rows)
        col = ids_col[pl.ds(start, step_rows), :]
        for j in range(stations // LANES):
            lane = slice(j * LANES, (j + 1) * LANES)
            sid = lax.broadcasted_iota(jnp.int32, (step_rows, LANES), 1) + j * LANES
            scatter_hot[pl.ds(start, step_rows), lane] = jnp.where(sid == col, 1.0, 0.0).astype(jnp.bfloat16)
        return carry

    lax.fori_loop(0, 2 * base // step_rows, hot_body2, 0)

    pl.semaphore_wait(barrier, n_band - 1 + stages)

    row_copies = []
    for step in range(1, n_band):
        copy = pltpu.make_async_remote_copy(
            src_ref=row,
            dst_ref=rows_all.at[step],
            send_sem=row_send.at[step],
            recv_sem=row_recv.at[step],
            device_id={"band": lax.rem(me + step, n_band)},
            device_id_type=MESH,
        )
        copy.start()
        row_copies.append(copy)

    loads[0].wait()

    pairs = [(a, b) for a in range(4) for b in range(a, 4)]

    def gram_body(j, carry):
        lane = pl.ds(pl.multiple_of(j * LANES, LANES), LANES)
        for k in range(dirs):
            c = [
                [coh[k, v, h * SUB : (h + 1) * SUB, lane] for h in range(halves)]
                for v in range(8)
            ]
            for n, (a, b) in enumerate(pairs):
                real = sum(c[a][h] * c[b][h] + c[4 + a][h] * c[4 + b][h] for h in range(halves))
                grams[(2 * n) * dirs + k : (2 * n) * dirs + k + 1, lane] = jnp.sum(real, axis=0, keepdims=True)
                if a != b:
                    imag = sum(c[4 + a][h] * c[b][h] - c[a][h] * c[4 + b][h] for h in range(halves))
                    grams[(2 * n + 1) * dirs + k : (2 * n + 1) * dirs + k + 1, lane] = jnp.sum(
                        imag, axis=0, keepdims=True
                    )
        return carry

    lax.fori_loop(0, blocks, gram_body, 0)

    def gram(a, b):
        if a > b:
            return conj(gram(b, a))
        n = pairs.index((a, b))
        real = grams[(2 * n) * dirs : (2 * n + 1) * dirs, :]
        if a == b:
            return real
        return (real, grams[(2 * n + 1) * dirs : (2 * n + 2) * dirs, :])

    def start_consensus():
        loads[1].wait()
        loads[2].wait()
        for k in range(dirs):
            for v in range(8):
                total = basis[0, 0] * coeffs0[(0,) + halves_of(k, v)]
                for m in range(1, SUB):
                    total = total + basis[0, m] * coeffs0[(m,) + halves_of(k, v)]
                cons[packed(k, v), :] = total

    def solve_weights():
        for copy in row_copies:
            copy.wait()
        rows_all[0] = row[...]
        held = [rows_all[s] for s in range(n_band)]
        columns = []
        for m in range(SUB):
            total = held[0] * held[0][m : m + 1, :]
            for s in range(1, n_band):
                total = total + held[s] * held[s][m : m + 1, :]
            ident = jnp.where(lax.broadcasted_iota(jnp.int32, (SUB, LANES), 0) == m, RIDGE * n_band, 0.0)
            columns.append(total + ident.astype(f32))
        right = list(held)
        iota = lax.broadcasted_iota(jnp.int32, (SUB, LANES), 0)
        for i in range(SUB):
            inverse = 1.0 / columns[i][i : i + 1, :]
            factor = columns[i]
            for group in (columns, right):
                for c in range(len(group)):
                    lead = jnp.broadcast_to(group[c][i : i + 1, :] * inverse, (SUB, LANES))
                    group[c] = jnp.where(iota == i, lead, group[c] - factor * lead)
        for s in range(n_band):
            band = lax.rem(me + n_band - s, n_band)
            gweights[band] = right[s]
            weights[band] = jnp.broadcast_to(
                jnp.sum(right[s] * held[0], axis=0, keepdims=True), (SUB, LANES)
            )

    x_copies = [{} for _ in range(ITERS)]

    ahead = n_band // 2
    behind = n_band - 1 - ahead

    def slot_of(way, distance):
        if distance > behind:
            return n_band - 1
        return distance + way * behind if distance else 0

    def reach_of(k, way):
        return ahead if way == k % 2 else behind

    def send_x(turn, k, way, distance):
        to = slot_of(way, distance + 1)
        copy = pltpu.make_async_remote_copy(
            src_ref=xall.at[turn, k, slot_of(way, distance)],
            dst_ref=xall.at[turn, k, to],
            send_sem=x_send.at[turn, k, to - 1],
            recv_sem=x_recv.at[turn, k, to - 1],
            device_id={"band": nexts[way]},
            device_id_type=MESH,
        )
        copy.start()
        x_copies[turn][(k, way, distance + 1)] = copy

    def pump(turn, distance, chosen=range(dirs)):
        for k in chosen:
            for way in range(2):
                reach = reach_of(k, way)
                if distance <= reach:
                    x_copies[turn][(k, way, distance)].wait_recv()
                    if distance < reach:
                        send_x(turn, k, way, distance)

    def source(slot):
        if slot <= behind:
            return at(lax.rem(pos + n_band - slot, n_band))
        return at(lax.rem(pos + slot - behind, n_band))

    def end(comp, lane):
        return ends[comp * dirs : (comp + 1) * dirs, lane]

    early, late = range(dirs // 2), range(dirs // 2, dirs)
    d_copies = []

    def send_d(turn, n, src, dst, stage):
        copy = pltpu.make_async_remote_copy(
            src_ref=src,
            dst_ref=dst,
            send_sem=d_send.at[turn, n],
            recv_sem=d_recv.at[turn, n],
            device_id={"dir": flip(stage)},
            device_id_type=MESH,
        )
        copy.start()
        d_copies.append(copy)
        return copy

    first = slice(0, base)
    second = slice(base, 2 * base)

    for turn in range(ITERS):
        for g in range(nrow // SUB):
            for j in range(per):
                value = jones[pl.ds(g * SUB * per + j, SUB, stride=per), :]
                left = value
                for piece in range(PIECES):
                    part = left.astype(jnp.bfloat16)
                    lhs[
                        piece * nrow + g * SUB : piece * nrow + (g + 1) * SUB,
                        j * LANES : (j + 1) * LANES,
                    ] = part
                    left = left - part.astype(f32)
        ends[...] = join(jnp.dot(lhs[...], gather_hot[...], preferred_element_type=f32), nrow)

        def model_body(i, carry):
            j = i // halves
            h = lax.rem(i, halves)
            lane = pl.ds(pl.multiple_of(j * LANES, LANES), LANES)
            lane_q = pl.ds(pl.multiple_of(base + j * LANES, LANES), LANES)
            time = pl.ds(pl.multiple_of(h * SUB, SUB), SUB)
            total = [None] * 4
            for k in range(dirs):
                c = [(coh[k, v, time, lane], coh[k, 4 + v, time, lane]) for v in range(4)]

                def spread(v, where):
                    return tuple(
                        jnp.broadcast_to(
                            ends[(4 * part + v) * dirs + k : (4 * part + v) * dirs + k + 1, where],
                            (SUB, LANES),
                        )
                        for part in range(2)
                    )

                p = [spread(v, lane) for v in range(4)]
                q = [spread(v, lane_q) for v in range(4)]
                for a in range(2):
                    b = [cadd(cmul(p[2 * a], c[d]), cmul(p[2 * a + 1], c[2 + d])) for d in range(2)]
                    for d in range(2):
                        term = cadd(cmul_conj(b[0], q[2 * d]), cmul_conj(b[1], q[2 * d + 1]))
                        v = 2 * a + d
                        total[v] = term if total[v] is None else cadd(total[v], term)
            for v in range(4):
                model[turn, 0, v, time, lane] = total[v][0]
                model[turn, 1, v, time, lane] = total[v][1]
            return carry

        lax.fori_loop(0, blocks * halves, model_body, 0)

        other = 1 - own
        hop = send_d(turn, 0, model.at[turn, other], got_a.at[turn], 0)
        jp = [(end(v, first), end(4 + v, first)) for v in range(4)]
        jq = [(end(v, second), end(4 + v, second)) for v in range(4)]

        def gram_of(j):
            m00 = re_mul(j[0], conj(j[0])) + re_mul(j[2], conj(j[2]))
            m11 = re_mul(j[1], conj(j[1])) + re_mul(j[3], conj(j[3]))
            m01 = cadd(cmul_conj(j[1], j[0]), cmul_conj(j[3], j[2]))
            return m00, m11, m01

        m00, m11, m01 = gram_of(jq)
        p00, p11, p01 = gram_of(jp)
        n1_00 = m00 * gram(0, 0) + m11 * gram(1, 1) + 2.0 * re_mul(m01, gram(0, 1))
        n1_11 = m00 * gram(2, 2) + m11 * gram(3, 3) + 2.0 * re_mul(m01, gram(2, 3))
        n1_01 = cadd(
            cadd(scale(m00, gram(0, 2)), scale(m11, gram(1, 3))),
            cadd(cmul(m01, gram(0, 3)), cmul(conj(m01), gram(1, 2))),
        )
        n2_00 = p00 * gram(0, 0) + p11 * gram(2, 2) + 2.0 * re_mul(p01, gram(2, 0))
        n2_11 = p00 * gram(1, 1) + p11 * gram(3, 3) + 2.0 * re_mul(p01, gram(3, 1))
        n2_01 = cadd(
            cadd(scale(p00, gram(1, 0)), scale(p11, gram(3, 2))),
            cadd(cmul(p01, gram(3, 0)), cmul(conj(p01), gram(1, 2))),
        )
        for n, (left, right) in enumerate(
            ((n1_00, n2_00), (n1_11, n2_11), (n1_01[0], n2_01[0]), (n1_01[1], n2_01[1]))
        ):
            vals_n[n * dirs : (n + 1) * dirs, first] = left
            vals_n[n * dirs : (n + 1) * dirs, second] = right

        if turn > 0:
            pump(turn - 1, 1, early)
        hop.wait_recv()
        sum_a[turn, 0] = model[turn, own] + got_a[turn]
        for stage in range(1, stages):
            hop = send_d(turn, stage, sum_a.at[turn, stage - 1], got_b.at[turn, stage - 1], stage)
            if stage == 1:
                if turn > 0:
                    pump(turn - 1, 1, late)
                split_store(lhs_n, 4 * dirs, vals_n[...])
                found = join(jnp.dot(lhs_n[...], scatter_hot[...], preferred_element_type=f32), 4 * dirs)
                for g in range(4 * dirs // SUB):
                    for j in range(per):
                        seg_n[pl.ds(g * SUB * per + j, SUB, stride=per), :] = found[
                            g * SUB : (g + 1) * SUB, j * LANES : (j + 1) * LANES
                        ]
                if turn == 0:
                    start_consensus()
                    solve_weights()
                else:
                    for s in range(2, (ahead + 2) // 2):
                        pump(turn - 1, s)
            hop.wait_recv()
            target = sum_a.at[turn, stage] if stage + 1 < stages else sum_b.at[turn]
            target[...] = sum_a[turn, stage - 1] + got_b[turn, stage - 1]
        hop = send_d(turn, stages, sum_b.at[turn], got_c.at[turn], 0)
        if turn > 0:
            for s in range(max(2, (ahead + 2) // 2), ahead):
                pump(turn - 1, s, early if s + 1 == ahead else range(dirs))
        res[own] = vis[own] - sum_b[turn]
        hop.wait_recv()
        res[other] = vis[other] - got_c[turn]
        if turn > 0 and ahead - 1 >= max(2, (ahead + 2) // 2):
            pump(turn - 1, ahead - 1, late)

        def cross_body(j, carry):
            lane = pl.ds(pl.multiple_of(j * LANES, LANES), LANES)
            r = [[res[v // 4, v % 4, h * SUB : (h + 1) * SUB, lane] for h in range(halves)] for v in range(8)]
            for k in range(dirs):
                c = [[coh[k, v, h * SUB : (h + 1) * SUB, lane] for h in range(halves)] for v in range(8)]
                for a in range(4):
                    for b in range(4):
                        real = sum(r[a][h] * c[b][h] + r[4 + a][h] * c[4 + b][h] for h in range(halves))
                        imag = sum(r[4 + a][h] * c[b][h] - r[a][h] * c[4 + b][h] for h in range(halves))
                        n = 2 * (4 * a + b)
                        cross[n * dirs + k : n * dirs + k + 1, lane] = jnp.sum(real, axis=0, keepdims=True)
                        cross[(n + 1) * dirs + k : (n + 1) * dirs + k + 1, lane] = jnp.sum(
                            imag, axis=0, keepdims=True
                        )
            return carry

        lax.fori_loop(0, blocks, cross_body, 0)

        def crossed(a, b):
            n = 2 * (4 * a + b)
            return (
                cross[n * dirs : (n + 1) * dirs, :],
                cross[(n + 1) * dirs : (n + 2) * dirs, :],
            )

        def herm(which):
            zero = [vals_n[n * dirs : (n + 1) * dirs, which] for n in range(4)]
            return zero[0], zero[1], (zero[2], zero[3])

        for which, j, other_end in ((first, jq, jp), (second, jp, jq)):
            h00, h11, h01 = herm(which)
            for a in range(2):
                for c in range(2):
                    total = None
                    for b in range(2):
                        for d in range(2):
                            if which is first:
                                term = cmul(j[2 * b + d], crossed(2 * a + b, 2 * c + d))
                            else:
                                term = cmul_conj(j[2 * b + d], crossed(2 * b + a, 2 * d + c))
                            total = term if total is None else cadd(total, term)
                    if c == 0:
                        extra = cadd(scale(h00, other_end[2 * a]), cmul_conj(other_end[2 * a + 1], h01))
                    else:
                        extra = cadd(cmul(other_end[2 * a], h01), scale(h11, other_end[2 * a + 1]))
                    total = cadd(total, extra)
                    for part in range(2):
                        n = 4 * part + 2 * a + c
                        vals[n * dirs : (n + 1) * dirs, which] = total[part]

        split_store(lhs, nrow, vals[...])
        found = join(jnp.dot(lhs[...], scatter_hot[...], preferred_element_type=f32), nrow)
        for g in range(nrow // SUB):
            for j in range(per):
                seg[pl.ds(g * SUB * per + j, SUB, stride=per), :] = found[
                    g * SUB : (g + 1) * SUB, j * LANES : (j + 1) * LANES
                ]

        def join_bands(previous):
            pump(previous, ahead)
            for k in range(dirs):
                for v in range(8):
                    here = pl.ds((v * dirs + k) * per, per)
                    total = None
                    for s in range(n_band):
                        term = weights[source(s)] * xall[previous, k, s, v]
                        total = term if total is None else total + term
                    cons[here, :] = total
                    fresh = dual[here, :] + RHO * (jones[here, :] - total)
                    if previous + 1 < ITERS:
                        dual[here, :] = fresh
                    else:
                        dual_out[halves_of(k, v)] = fresh

        if turn > 0:
            join_bands(turn - 1)

        for k in range(dirs):
            def rows_of(v):
                return pl.ds((v * dirs + k) * per, per)

            y = []
            for v in range(8):
                here = rows_of(v)
                y.append(seg[here, :] + RHO * cons[here, :] - dual[here, :])
            h00, h11, re01, im01 = [seg_n[rows_of(n), :] for n in range(4)]
            h00 = h00 + RHO
            h11 = h11 + RHO
            inverse = 1.0 / (h00 * h11 - (re01 * re01 + im01 * im01))
            h00, h11, h01 = h00 * inverse, h11 * inverse, (re01 * inverse, im01 * inverse)
            for a in range(2):
                y0, y1 = (y[2 * a], y[4 + 2 * a]), (y[2 * a + 1], y[4 + 2 * a + 1])
                minus0, minus1 = cmul_conj(y1, h01), cmul(y0, h01)
                for part in range(2):
                    for c in range(2):
                        if c == 0:
                            value = h11 * y0[part] - minus0[part]
                        else:
                            value = h00 * y1[part] - minus1[part]
                        v = 4 * part + 2 * a + c
                        here = rows_of(v)
                        jones[here, :] = value
                        if turn + 1 == ITERS:
                            jones_out[halves_of(k, v)] = value
                        xall[turn, k, 0, v] = value + dual[here, :] * (1.0 / RHO)
            for way in range(2):
                if reach_of(k, way):
                    send_x(turn, k, way, 0)

    last = ITERS - 1
    for s in range(1, ahead):
        pump(last, s)
    join_bands(last)

    def coeff_body(m, carry):
        for k in range(dirs):
            total = [None] * 8
            for s in range(n_band):
                factor = jnp.broadcast_to(gweights[source(s), pl.ds(m, 1), :], (SUB, LANES))
                for v in range(8):
                    term = factor * xall[last, k, s, v]
                    total[v] = term if total[v] is None else total[v] + term
            for v in range(8):
                coeffs[(m,) + halves_of(k, v)] = total[v]
        return carry

    lax.fori_loop(0, SUB, coeff_body, 0)

    for copies in x_copies:
        for copy in copies.values():
            copy.wait_send()
    for copy in d_copies:
        copy.wait_send()


def local(n_band, n_dir, vis, coh, jones_start, dual_start, consensus_start, freq_basis, pairs):
    f32 = jnp.float32
    dirs, times, base = coh.shape[1], coh.shape[-2], coh.shape[-1]
    stations = jones_start.shape[-1]
    per = stations // LANES
    nrow = 8 * dirs
    terms = freq_basis.shape[1]

    def enter(value):
        lead = value.shape[:-2]
        value = value.reshape(lead + (2, per, LANES))
        return jnp.swapaxes(value, -2, -3).reshape(lead + (2 * per, LANES))

    def leave(value, shape):
        value = value.reshape(value.shape[:-2] + (per, 2, LANES))
        return jnp.swapaxes(value, -2, -3).reshape(shape)

    stages = n_dir.bit_length() - 1
    half = (4, times, base)
    vmem = pl.BlockSpec(memory_space=pltpu.VMEM)
    far = pl.BlockSpec(memory_space=pl.ANY)
    raw = (dirs, 4, 2 * per, LANES)
    raw_out = jax.ShapeDtypeStruct(raw, f32)
    bf16 = jnp.bfloat16
    jones, dual, coeffs = pl.pallas_call(
        functools.partial(kernel, n_band, n_dir, dirs, times, base, stations),
        out_shape=(raw_out, raw_out, jax.ShapeDtypeStruct((terms,) + raw, f32)),
        in_specs=[far, far, vmem, vmem, far, pl.BlockSpec(memory_space=pltpu.SMEM), vmem],
        out_specs=(vmem,) * 3,
        scratch_shapes=[
            pltpu.VMEM((2,) + half, f32),
            pltpu.VMEM((dirs, 8, times, base), f32),
            pltpu.VMEM((terms,) + raw, f32),
            pltpu.VMEM((nrow * per, LANES), f32),
            pltpu.VMEM((nrow * per, LANES), f32),
            pltpu.VMEM((SUB, LANES), f32),
            pltpu.VMEM((2 * base, LANES), jnp.int32),
            pltpu.VMEM((nrow * per, LANES), f32),
            pltpu.VMEM((ITERS, dirs, n_band, 8, per, LANES), f32),
            pltpu.VMEM((n_band, SUB, LANES), f32),
            pltpu.VMEM((n_band, SUB, LANES), f32),
            pltpu.VMEM((n_band, SUB, LANES), f32),
            pltpu.VMEM((stations, 2 * base), bf16),
            pltpu.VMEM((2 * base, stations), bf16),
            pltpu.VMEM((PIECES * nrow, max(stations, 2 * base)), bf16),
            pltpu.VMEM((PIECES * 4 * dirs, 2 * base), bf16),
            pltpu.VMEM((nrow, 2 * base), f32),
            pltpu.VMEM((20 * dirs, base), f32),
            pltpu.VMEM((32 * dirs, base), f32),
            pltpu.VMEM((nrow, 2 * base), f32),
            pltpu.VMEM((4 * dirs, 2 * base), f32),
            pltpu.VMEM((nrow * per, LANES), f32),
            pltpu.VMEM((4 * dirs * per, LANES), f32),
            pltpu.VMEM((ITERS, 2) + half, f32),
            pltpu.VMEM((ITERS,) + half, f32),
            pltpu.VMEM((ITERS, stages - 1) + half, f32),
            pltpu.VMEM((ITERS, stages - 1) + half, f32),
            pltpu.VMEM((ITERS,) + half, f32),
            pltpu.VMEM((ITERS,) + half, f32),
            pltpu.VMEM((2,) + half, f32),
            pltpu.SemaphoreType.DMA((3,)),
            pltpu.SemaphoreType.DMA((n_band,)),
            pltpu.SemaphoreType.DMA((n_band,)),
            pltpu.SemaphoreType.DMA((ITERS, dirs, n_band - 1)),
            pltpu.SemaphoreType.DMA((ITERS, dirs, n_band - 1)),
            pltpu.SemaphoreType.DMA((ITERS, stages + 1)),
            pltpu.SemaphoreType.DMA((ITERS, stages + 1)),
        ],
        compiler_params=pltpu.CompilerParams(
            collective_id=0, has_side_effects=True, vmem_limit_bytes=60 * 1024 * 1024
        ),
    )(
        vis.reshape((2,) + half),
        coh.reshape(dirs, 8, times, base),
        enter(jones_start.reshape((dirs, 4, 2, stations))),
        enter(dual_start.reshape((dirs, 4, 2, stations))),
        enter(consensus_start.reshape((terms, dirs, 4, 2, stations))),
        freq_basis,
        pairs,
    )
    return (
        leave(jones, jones_start.shape),
        leave(dual, jones_start.shape),
        leave(coeffs, consensus_start.shape),
    )


def solution(mesh):
    in_specs = (
        P("band", None, None, None, None, None),
        P("band", "dir", None, None, None, None, None),
        P("band", "dir", None, None, None, None),
        P("band", "dir", None, None, None, None),
        P(None, "dir", None, None, None, None),
        P("band", None),
        P(),
    )
    out_specs = (
        P("band", "dir", None, None, None, None),
        P("band", "dir", None, None, None, None),
        P(None, "dir", None, None, None, None),
    )
    body = functools.partial(local, mesh.shape["band"], mesh.shape["dir"])
    return jax.shard_map(body, mesh=mesh, in_specs=in_specs, out_specs=out_specs, check_vma=False)
```
